512 devices in a mesh: dp: 64 (over y_lo, z, core), shard: 8 (over y_hi, x).
Axes of the slice: x: 4, y: 8 (y_hi: 2, y_lo: 4; y = y_hi * 4 + y_lo), z: 8, core: 2. Of those that a mesh axis runs over, the one named last changes fastest.
Arguments:
- hidden: bfloat16 [131072, 2560], P(('dp', 'shard')), may hold values from -6 to 6
- resid: bfloat16 [1280, 131072], P('shard', 'dp'), may hold values from -6 to 6
- target: bfloat16 [1280, 131072], P('shard', 'dp'), may hold values from -6 to 6
- w_out: bfloat16 [1280, 2560], P('shard'), may hold values from -0.125 to 0.125
- signs: int32 [40, 2560], P('shard'), may hold values from -2147483648 to 2147483646
- m_old: float32 [25600, 128], P(('shard', 'dp')), may hold values from -4 to 4
- v_old: float32 [25600, 128], P(('shard', 'dp')), may hold values from 13.1072 to 131.072
Outputs:
- new_w: bfloat16 [1280, 2560], P('shard')
- new_m: float32 [25600, 128], P(('shard', 'dp'))
- new_v: float32 [25600, 128], P(('shard', 'dp'))
The draws below stay inside these ranges and needn't reach their ends.
Inputs may be any that keep to these rules, and one draw needn't show every extreme that they name: Every word carries 32 independent signs, bit b of word k belonging to output feature 32 k + b.
All inputs are finite; a program needn't handle non-finite values.
Results may differ from the reference program's by a relative error of at most 0.0023.
Values may be sent and summed in bfloat16 or wider, within the bound.
No kernel may reach another device: no remote copies, remote signals or barrier semaphores. Data moves between devices by JAX's collectives and lax.ppermute only.
A program may use at most 64 MiB of HBM per device.

```python
import math
import jax
import jax.numpy as jnp
from jax import lax

D = 1280
HID = 2560
TOK_DEV = 256
OPT_STEP = 10
TOKENS = 131072
N_DP = 64
N_SHARD = 8


def place_ends(values, stream_key, smallest, top_value):
    spot = [jax.random.randint(jax.random.fold_in(stream_key, axis), (), 0, length) for axis, length in enumerate(values.shape)]
    longest = values.shape.index(max(values.shape))
    beside = spot[:longest] + [(spot[longest] + 1) % values.shape[longest]] + spot[longest + 1:]
    return values.at[tuple(spot)].set(smallest).at[tuple(beside)].set(top_value)


def block_levels(key, dims, pieces, smallest, top_value):
    level = 1.0
    for position, shards_of in pieces:
        draws = jax.random.uniform(jax.random.fold_in(jax.random.fold_in(key, 6), position), (shards_of,), jnp.float32, smallest / len(pieces), top_value / len(pieces))
        level = level * jnp.repeat(jnp.exp(draws), dims[position] // shards_of).reshape((-1,) + (1,) * (len(dims) - 1 - position))
    return level


def noise(key, dims, scale, reach, split=(), kind=jnp.bfloat16):
    gain = block_levels(key, dims, split, -0.22, 0.18) if split else 1.0
    values = jax.random.normal(key, dims, jnp.float32) * scale * gain
    return jnp.minimum(jnp.maximum(values, -reach), reach).astype(kind)


def setup_inputs(seed: int = 0) -> dict:
    splits = jax.random.split(jax.random.key(seed), 8)
    return {
        "hidden": noise(splits[0], (TOKENS, HID), 1.0, 6.0, ((0, 512),)),
        "resid": noise(splits[1], (D, TOKENS), 1.0, 6.0, ((0, 8), (1, 64))),
        "target": noise(splits[2], (D, TOKENS), 1.0, 6.0, ((0, 8), (1, 64))),
        "w_out": noise(splits[3], (D, HID), HID ** -0.5, 0.125, ((0, 8),)),
        "signs": place_ends(jax.random.randint(splits[4], (D // 32, HID), -2147483648, 2147483647), jax.random.fold_in(splits[4], 1), -2147483648, 2147483646).astype(jnp.int32),
        "m_old": noise(splits[5], (D * HID // 128, 128), 0.6, 4.0, ((0, 512),), jnp.float32),
        "v_old": jnp.clip(jnp.exp(math.log(131.072) - 2.3025852 * jax.random.uniform(splits[6], (D * HID // 128, 128), jnp.float32) ** block_levels(splits[6], (D * HID // 128, 128), ((0, 512),), -0.2, 0.2)), 13.1072, 131.072),
    }


def unpack_signs(signs):
    shifts = jnp.arange(32, dtype=jnp.int32)
    bit_values = jnp.bitwise_and(jnp.right_shift(signs[:, None, :], shifts[None, :, None]), 1)
    return (1 - 2 * bit_values).reshape(signs.shape[0] * 32, signs.shape[1]).astype(jnp.bfloat16)

def reference(hidden, resid, target, w_out, signs, m_old, v_old):
    probes = unpack_signs(signs)
    group_size = TOK_DEV * N_SHARD
    blocks = hidden.reshape(N_DP, group_size, HID)
    resid_blocks = jnp.transpose(resid.reshape(D, N_DP, group_size), (1, 0, 2))
    target_blocks = jnp.transpose(target.reshape(D, N_DP, group_size), (1, 0, 2))
    stacked = jnp.concatenate([w_out, probes], axis=0)

    def accumulate(running, block_items):
        hidden_block, resid_block, target_block = block_items
        forward = lax.dot_general(stacked, hidden_block, (((1,), (1,)), ((), ())), preferred_element_type=jnp.float32)
        output = forward[:D]
        tangent = forward[D:]
        misfit = resid_block.astype(jnp.float32) + output - target_block.astype(jnp.float32)
        spread = 1.0 + misfit * misfit
        rooted = jnp.sqrt(spread)
        slopes = (misfit / rooted).astype(jnp.bfloat16)
        bends = (tangent / (spread * rooted)).astype(jnp.bfloat16)
        grad_part = jnp.dot(slopes, hidden_block, preferred_element_type=jnp.float32)
        curve_part = jnp.dot(bends, hidden_block, preferred_element_type=jnp.float32)
        return ((running[0] + grad_part, running[1] + curve_part), None)
    empty = jnp.zeros((D, HID), jnp.float32)
    (grad_sum, curve_sum), _ = lax.scan(accumulate, (empty, empty), (blocks, resid_blocks, target_blocks))
    scaling = 1.0 / math.sqrt(TOKENS)
    gradient = (grad_sum * scaling).reshape(D * HID // 128, 128)
    curvature = (curve_sum * scaling).reshape(D * HID // 128, 128)
    diag_est = probes.astype(jnp.float32).reshape(D * HID // 128, 128) * curvature
    new_m = 0.9 * m_old + 0.1 * gradient
    new_v = 0.999 * v_old + 0.001 * diag_est * diag_est
    first_fix = 1.0 - 0.9 ** OPT_STEP
    second_fix = 1.0 - 0.999 ** OPT_STEP
    update = new_m / first_fix / (jnp.sqrt(new_v / second_fix) + 0.0001)
    new_w = (w_out.astype(jnp.float32) - 0.15 * update.reshape(D, HID)).astype(jnp.bfloat16)
    return (new_w, new_m, new_v)
```

```python
import math

import jax
import jax.numpy as jnp
from jax import lax
from jax.sharding import Mesh, PartitionSpec as P

OPT_STEP = 10


beta_one = 0.9
beta_two = 0.999
learn_rate = 0.15
epsilon = 0.0001


def size(axis):
    return 8 if axis == "y" else lax.axis_size(axis)


def place(axis):
    if axis == "y":
        return lax.axis_index("yh") * 4 + lax.axis_index("yl")
    return lax.axis_index(axis)


def shift(value, axis, by):
    n = size(axis)
    hops = [(i, (i + by) % n) for i in range(n)]
    if axis == "y":
        at = [2 * (y % 4) + y // 4 for y in range(n)]
        return lax.ppermute(value, ("yl", "yh"), [(at[i], at[j]) for i, j in hops])
    return lax.ppermute(value, axis, hops)


def unpack_signs(signs):
    shifts = jnp.arange(32, dtype=jnp.int32)
    bit_values = jnp.bitwise_and(jnp.right_shift(signs[:, None, :], shifts[None, :, None]), 1)
    return (1 - 2 * bit_values).reshape(signs.shape[0] * 32, signs.shape[1]).astype(jnp.bfloat16)


def exchange_sum(pieces, axis, wire):
    n = size(axis)
    me = place(axis)
    total = lax.dynamic_index_in_dim(pieces, me, 0, keepdims=False)
    arrived = []
    for by in range(1, n):
        piece = lax.dynamic_index_in_dim(pieces, (me + by) % n, 0, keepdims=False)
        arrived.append(shift(piece.astype(wire), axis, by))
    for term in arrived:
        total = total + term.astype(jnp.float32)
    return total


def exchange_blocks(block, axis):
    n = lax.axis_size(axis)
    me = lax.axis_index(axis)
    blocks = [block] + [shift(block, axis, by) for by in range(1, n)]
    stacked = jnp.stack(blocks[:1] + blocks[:0:-1])
    return jnp.roll(stacked, me, axis=0)


def on_device(hidden, resid, target, w_out, signs, m_old, v_old):
    features, width = w_out.shape
    tokens = hidden.shape[0]
    group = tokens * lax.axis_size("x")
    half = lax.axis_index("yh")
    core = lax.axis_index("c")
    col = lax.axis_index("x")

    from_left = shift(hidden, "x", 1)
    from_right = shift(hidden, "x", -1)
    far_top = shift(from_left[: tokens // 2], "x", 1)
    far_low = shift(from_right[tokens // 2 :], "x", -1)

    pair = jnp.stack([resid, target])
    other_pair = shift(lax.dynamic_slice_in_dim(pair, (1 - half) * group, group, 2), "yh", 1)
    other_signs = shift(signs, "yh", 1)
    rows = features // 2
    part = shift(lax.dynamic_slice_in_dim(w_out, core * rows, rows, 0), "yh", 1)
    twin = shift(part, "c", 1)
    other_w = jnp.concatenate(
        [jnp.where(core == 0, part, twin), jnp.where(core == 0, twin, part)], axis=0
    )
    probes = unpack_signs(signs)
    other_probes = unpack_signs(other_signs)
    own_pair = lax.dynamic_slice_in_dim(pair, half * group, group, 2)

    def in_order(own, other):
        first = jnp.where(half == 0, own, other)
        second = jnp.where(half == 0, other, own)
        return jnp.concatenate([first, second], axis=0)

    stacked = jnp.concatenate([in_order(w_out, other_w), in_order(probes, other_probes)], axis=0)
    pair_all = jnp.concatenate(
        [jnp.where(half == 0, own_pair, other_pair), jnp.where(half == 0, other_pair, own_pair)], axis=1
    )
    count = 2 * features

    def run(block, places):
        cols = [lax.dynamic_slice_in_dim(pair_all, ((col + k) % 4) * tokens, tokens, 2) for k in places]
        here = jnp.concatenate(cols, axis=2) if len(cols) > 1 else cols[0]
        forward = lax.dot_general(
            stacked, block, (((1,), (1,)), ((), ())), preferred_element_type=jnp.float32
        )
        misfit = here[0].astype(jnp.float32) + forward[:count] - here[1].astype(jnp.float32)
        spread = 1.0 + misfit * misfit
        rooted = jnp.sqrt(spread)
        slopes = (misfit / rooted).astype(jnp.bfloat16)
        bends = (forward[count:] / (spread * rooted)).astype(jnp.bfloat16)
        away = jnp.where(core == 0, bends, slopes)
        kept = jnp.where(core == 0, slopes, bends)
        return away, kept

    near = jnp.concatenate([hidden, from_left, from_right], axis=0)
    away_near, kept_near = run(near, (0, 3, 1))
    sum_away = jnp.dot(away_near, near, preferred_element_type=jnp.float32)
    sum_kept = jnp.dot(kept_near, near, preferred_element_type=jnp.float32)
    far = jnp.concatenate([far_top, far_low], axis=0)
    away_far, kept_far = run(far, (2,))
    sum_away = sum_away + jnp.dot(away_far, far, preferred_element_type=jnp.float32)
    got = shift(sum_away, "c", 1)
    sum_kept = sum_kept + jnp.dot(kept_far, far, preferred_element_type=jnp.float32)
    mine = sum_kept + got

    across, deep = 8, lax.axis_size("z")
    per = count * width // (across * deep * 128)
    pieces = jnp.moveaxis(mine.reshape(across, deep, per, 128), 1, 0)
    over_z = exchange_sum(pieces, "z", jnp.bfloat16)
    over_y = exchange_sum(over_z, "y", jnp.float32)
    each = per // 2
    keep_rows = lax.dynamic_slice_in_dim(over_y, core * each, each, 0)
    send_rows = lax.dynamic_slice_in_dim(over_y, (1 - core) * each, each, 0)
    got_rows = shift(send_rows, "c", 1)
    grad_mine = jnp.where(core == 0, keep_rows, got_rows)
    curve_mine = jnp.where(core == 0, got_rows, keep_rows)

    scaling = 1.0 / math.sqrt(tokens * 512)
    gradient = grad_mine * scaling
    curvature = curve_mine * scaling
    row_start = (
        (lax.axis_index("yl") * lax.axis_size("z") + lax.axis_index("z")) * 2 + core
    ) * each
    my_probes = lax.dynamic_slice_in_dim(probes.reshape(-1, 128), row_start, each, 0)
    diag_est = my_probes.astype(jnp.float32) * curvature
    new_m = beta_one * m_old + (1.0 - beta_one) * gradient
    new_v = beta_two * v_old + (1.0 - beta_two) * diag_est * diag_est
    first_fix = 1.0 - beta_one**OPT_STEP
    second_fix = 1.0 - beta_two**OPT_STEP
    update = new_m / first_fix / (jnp.sqrt(new_v / second_fix) + epsilon)
    own_rows = lax.dynamic_slice_in_dim(w_out.reshape(-1, 128), row_start, each, 0)
    fresh = (own_rows.astype(jnp.float32) - learn_rate * update).astype(jnp.bfloat16)

    by_y = exchange_blocks(fresh, "yl")
    by_z = exchange_blocks(by_y, "z")
    twin_z = shift(by_z, "c", 1)
    both = jnp.stack([jnp.where(core == 0, by_z, twin_z), jnp.where(core == 0, twin_z, by_z)])
    new_w = jnp.transpose(both, (2, 1, 0, 3, 4)).reshape(w_out.shape)
    return (new_w, new_m, new_v)


def solution(mesh):
    fine = Mesh(mesh.devices.reshape(4, 8, 2, 2, 4), ("yl", "z", "c", "yh", "x"))
    dp, shard = ("yl", "z", "c"), ("yh", "x")
    return jax.shard_map(
        on_device,
        mesh=fine,
        in_specs=(
            P(dp + shard, None),
            P(shard, dp),
            P(shard, dp),
            P(shard, None),
            P(shard, None),
            P(shard + dp, None),
            P(shard + dp, None),
        ),
        out_specs=(P(shard, None), P(shard + dp, None), P(shard + dp, None)),
        check_vma=False,
    )
```

```python
import math

import jax
import jax.numpy as jnp
from jax import lax
from jax.sharding import Mesh, PartitionSpec as P


OPT_STEP = 10


beta_one = 0.9
beta_two = 0.999
learn_rate = 0.15
epsilon = 0.0001


def size(axis):
    return 8 if axis == "y" else lax.axis_size(axis)


def shift(value, axis, by):
    n = size(axis)
    hops = [(i, (i + by) % n) for i in range(n)]
    if axis == "y":
        at = [2 * (y % 4) + y // 4 for y in range(n)]
        return lax.ppermute(value, ("yl", "yh"), [(at[i], at[j]) for i, j in hops])
    return lax.ppermute(value, axis, hops)


def unpack_signs(signs):
    shifts = jnp.arange(32, dtype=jnp.int32)
    bit_values = jnp.bitwise_and(jnp.right_shift(signs[:, None, :], shifts[None, :, None]), 1)
    return (1 - 2 * bit_values).reshape(signs.shape[0] * 32, signs.shape[1]).astype(jnp.bfloat16)


def step(hidden, resid, target, w_out, signs, m_old, v_old):
    features, width = w_out.shape
    tokens = hidden.shape[0]
    group = tokens * lax.axis_size("x")
    half = lax.axis_index("yh")
    core = lax.axis_index("c")
    col = lax.axis_index("x")
    odd = lax.axis_index("z") % 2

    from_left = shift(hidden, "x", 1)
    from_right = shift(hidden, "x", -1)

    quarter = features // 4
    piece = lax.dynamic_slice_in_dim(w_out, (core * 2 + odd) * quarter, quarter, 0)
    piece = shift(piece, "yh", 1)
    other_signs = shift(signs, "yh", 1)
    pair = jnp.stack([resid, target])
    other_pair = shift(lax.dynamic_slice_in_dim(pair, (1 - half) * group, group, 2), "yh", 1)
    beside = lax.ppermute(piece, "z", [(i, i ^ 1) for i in range(8)])
    part = jnp.concatenate(
        [jnp.where(odd == 0, piece, beside), jnp.where(odd == 0, beside, piece)], axis=0
    )
    twin = shift(part, "c", 1)
    other_w = jnp.concatenate(
        [jnp.where(core == 0, part, twin), jnp.where(core == 0, twin, part)], axis=0
    )
    far_top = shift(from_left[: tokens // 2], "x", 1)
    far_low = shift(from_right[tokens // 2 :], "x", -1)

    probes = unpack_signs(signs)
    other_probes = unpack_signs(other_signs)
    own_pair = lax.dynamic_slice_in_dim(pair, half * group, group, 2)

    def in_order(own, other):
        first = jnp.where(half == 0, own, other)
        second = jnp.where(half == 0, other, own)
        return jnp.concatenate([first, second], axis=0)

    stacked = jnp.concatenate([in_order(w_out, other_w), in_order(probes, other_probes)], axis=0)
    pair_all = jnp.concatenate(
        [jnp.where(half == 0, own_pair, other_pair), jnp.where(half == 0, other_pair, own_pair)], axis=1
    )
    count = 2 * features

    each = m_old.shape[0]
    row_start = (
        (lax.axis_index("yl") * lax.axis_size("z") + lax.axis_index("z")) * 2 + core
    ) * each
    my_probes = lax.dynamic_slice_in_dim(probes.reshape(-1, 128), row_start, each, 0)
    own_rows = lax.dynamic_slice_in_dim(w_out.reshape(-1, 128), row_start, each, 0)

    def run(block, places):
        cols = [lax.dynamic_slice_in_dim(pair_all, ((col + k) % 4) * tokens, tokens, 2) for k in places]
        here = jnp.concatenate(cols, axis=2) if len(cols) > 1 else cols[0]
        forward = lax.dot_general(
            stacked, block, (((1,), (1,)), ((), ())), preferred_element_type=jnp.float32
        )
        misfit = here[0].astype(jnp.float32) + forward[:count] - here[1].astype(jnp.float32)
        spread = 1.0 + misfit * misfit
        rooted = jnp.sqrt(spread)
        slopes = (misfit / rooted).astype(jnp.bfloat16)
        bends = (forward[count:] / (spread * rooted)).astype(jnp.bfloat16)
        away = jnp.where(core == 0, bends, slopes)
        kept = jnp.where(core == 0, slopes, bends)
        return away, kept

    near = jnp.concatenate([hidden, from_left, from_right], axis=0)
    away_near, kept_near = run(near, (0, 3, 1))
    sum_away = jnp.dot(away_near, near, preferred_element_type=jnp.float32)
    sum_kept = jnp.dot(kept_near, near, preferred_element_type=jnp.float32)
    sum_away, sum_kept, far_top, far_low, my_probes, own_rows = lax.optimization_barrier(
        (sum_away, sum_kept, far_top, far_low, my_probes, own_rows)
    )
    far = jnp.concatenate([far_top, far_low], axis=0)
    away_far, kept_far = run(far, (2,))
    sum_away = sum_away + jnp.dot(away_far, far, preferred_element_type=jnp.float32)
    got = shift(sum_away, "c", 1)
    sum_kept = sum_kept + jnp.dot(kept_far, far, preferred_element_type=jnp.float32)
    mine = (sum_kept + got).astype(jnp.bfloat16)

    plane = 64
    pieces = mine.reshape(plane, count * width // (plane * 128), 128)
    terms = lax.all_to_all(pieces, ("yh", "yl", "z"), 0, 0, tiled=True)
    total = jnp.sum(terms.astype(jnp.float32), axis=0)
    keep_rows = lax.dynamic_slice_in_dim(total, core * each, each, 0)
    send_rows = lax.dynamic_slice_in_dim(total, (1 - core) * each, each, 0)
    got_rows = shift(send_rows, "c", 1)
    grad_mine = jnp.where(core == 0, keep_rows, got_rows)
    curve_mine = jnp.where(core == 0, got_rows, keep_rows)

    scaling = 1.0 / math.sqrt(tokens * 512)
    gradient = grad_mine * scaling
    curvature = curve_mine * scaling
    diag_est = my_probes.astype(jnp.float32) * curvature
    new_m = beta_one * m_old + (1.0 - beta_one) * gradient
    new_v = beta_two * v_old + (1.0 - beta_two) * diag_est * diag_est
    first_fix = 1.0 - beta_one**OPT_STEP
    second_fix = 1.0 - beta_two**OPT_STEP
    update = new_m / first_fix / (jnp.sqrt(new_v / second_fix) + epsilon)
    fresh = (own_rows.astype(jnp.float32) - learn_rate * update).astype(jnp.bfloat16)

    spread_rows = jnp.broadcast_to(fresh[None], (32, *fresh.shape))
    mine_rows = lax.all_to_all(spread_rows, ("yl", "z"), 0, 0, tiled=True)
    twin_rows = shift(mine_rows, "c", 1)
    both = jnp.stack(
        [jnp.where(core == 0, mine_rows, twin_rows), jnp.where(core == 0, twin_rows, mine_rows)], axis=1
    )
    new_w = both.reshape(w_out.shape)
    return (new_w, new_m, new_v)


def solution(mesh):
    fine = Mesh(mesh.devices.reshape(4, 8, 2, 2, 4), ("yl", "z", "c", "yh", "x"))
    dp, shard = ("yl", "z", "c"), ("yh", "x")
    return jax.shard_map(
        step,
        mesh=fine,
        in_specs=(
            P(dp + shard, None),
            P(shard, dp),
            P(shard, dp),
            P(shard, None),
            P(shard, None),
            P(shard + dp, None),
            P(shard + dp, None),
        ),
        out_specs=(P(shard, None), P(shard + dp, None), P(shard + dp, None)),
        check_vma=False,
    )
```

```python
import math

import jax
import jax.numpy as jnp
from jax import lax
from jax.sharding import Mesh, PartitionSpec as P


OPT_STEP = 10


beta_one = 0.9
beta_two = 0.999
learn_rate = 0.15
epsilon = 0.0001


def size(axis):
    return 8 if axis == "y" else lax.axis_size(axis)


def shift(value, axis, by):
    n = size(axis)
    hops = [(i, (i + by) % n) for i in range(n)]
    if axis == "y":
        at = [2 * (y % 4) + y // 4 for y in range(n)]
        return lax.ppermute(value, ("yl", "yh"), [(at[i], at[j]) for i, j in hops])
    return lax.ppermute(value, axis, hops)


def unpack_signs(signs):
    shifts = jnp.arange(32, dtype=jnp.int32)
    bit_values = jnp.bitwise_and(jnp.right_shift(signs[:, None, :], shifts[None, :, None]), 1)
    return (1 - 2 * bit_values).reshape(signs.shape[0] * 32, signs.shape[1]).astype(jnp.bfloat16)


def step(hidden, resid, target, w_out, signs, m_old, v_old):
    features, width = w_out.shape
    tokens = hidden.shape[0]
    group = tokens * lax.axis_size("x")
    half = lax.axis_index("yh")
    core = lax.axis_index("c")
    col = lax.axis_index("x")
    odd = lax.axis_index("z") % 2

    from_left = shift(hidden, "x", 1)
    from_right = shift(hidden, "x", -1)

    quarter = features // 4
    piece = lax.dynamic_slice_in_dim(w_out, (core * 2 + odd) * quarter, quarter, 0)
    piece = shift(piece, "yh", 1)
    other_signs = shift(signs, "yh", 1)
    pair = jnp.stack(
        [lax.dynamic_slice_in_dim(part, (1 - half) * group, group, 1) for part in (resid, target)]
    )
    other_pair = shift(pair, "yh", 1)
    twin = shift(piece, "c", 1)
    beside = lax.ppermute(piece, "z", [(i, i ^ 1) for i in range(8)])
    across = lax.ppermute(piece, ("z", "c"), [(i, i ^ 3) for i in range(16)])
    far_top = shift(from_left[: tokens // 2], "x", 1)
    far_low = shift(from_right[tokens // 2 :], "x", -1)
    spot = core * 2 + odd
    other_w = jnp.zeros_like(w_out)
    for flip, rows in enumerate((piece, beside, twin, across)):
        other_w = lax.dynamic_update_slice_in_dim(other_w, rows, (spot ^ flip) * quarter, 0)
    other_stack = jnp.concatenate([other_w, unpack_signs(other_signs)], axis=0)
    probes = unpack_signs(signs)
    own_stack = jnp.concatenate([w_out, probes], axis=0)

    each = m_old.shape[0]
    row_start = (
        (lax.axis_index("yl") * lax.axis_size("z") + lax.axis_index("z")) * 2 + core
    ) * each
    my_probes = lax.dynamic_slice_in_dim(probes.reshape(-1, 128), row_start, each, 0)
    own_rows = lax.dynamic_slice_in_dim(w_out.reshape(-1, 128), row_start, each, 0)

    def run(stack, block, residual, wanted):
        forward = lax.dot_general(
            stack, block, (((1,), (1,)), ((), ())), preferred_element_type=jnp.float32
        )
        misfit = residual.astype(jnp.float32) + forward[:features] - wanted.astype(jnp.float32)
        spread = 1.0 + misfit * misfit
        rooted = jnp.sqrt(spread)
        slopes = (misfit / rooted).astype(jnp.bfloat16)
        bends = (forward[features:] / (spread * rooted)).astype(jnp.bfloat16)
        away = jnp.where(core == 0, bends, slopes)
        kept = jnp.where(core == 0, slopes, bends)
        return away, kept

    def columns(part, k, base):
        return lax.dynamic_slice_in_dim(part, base + ((col + k) % 4) * tokens, tokens, 1)

    def own_run(block, k):
        base = half * group
        return run(own_stack, block, columns(resid, k, base), columns(target, k, base))

    def other_run(block, k):
        return run(other_stack, block, columns(other_pair[0], k, 0), columns(other_pair[1], k, 0))

    def products(rows, block):
        return jnp.dot(rows, block, preferred_element_type=jnp.float32)

    near = ((hidden, 0), (from_left, 3), (from_right, 1))
    runs = [own_run(block, k) for block, k in near]
    away_own = sum(products(r[0], b) for r, (b, _) in zip(runs, near))
    kept_own = sum(products(r[1], b) for r, (b, _) in zip(runs, near))
    runs = [other_run(block, k) for block, k in near]
    away_other = sum(products(r[0], b) for r, (b, _) in zip(runs, near))
    kept_other = sum(products(r[1], b) for r, (b, _) in zip(runs, near))
    away_own, kept_own, away_other, kept_other, far_top, far_low, my_probes, own_rows = (
        lax.optimization_barrier(
            (away_own, kept_own, away_other, kept_other, far_top, far_low, my_probes, own_rows)
        )
    )
    far = jnp.concatenate([far_top, far_low], axis=0)
    own_far = own_run(far, 2)
    other_far = other_run(far, 2)
    got_own = shift(away_own + products(own_far[0], far), "c", 1)
    got_other = shift(away_other + products(other_far[0], far), "c", 1)
    mine_own = kept_own + products(own_far[1], far) + got_own
    mine_other = kept_other + products(other_far[1], far) + got_other
    mine = jnp.concatenate(
        [jnp.where(half == 0, mine_own, mine_other), jnp.where(half == 0, mine_other, mine_own)], axis=0
    ).astype(jnp.bfloat16)

    plane = 64
    pieces = mine.reshape(plane, 2 * features * width // (plane * 128), 128)
    terms = lax.all_to_all(pieces, ("yh", "yl", "z"), 0, 0, tiled=True)
    total = jnp.sum(terms.astype(jnp.float32), axis=0)
    keep_rows = lax.dynamic_slice_in_dim(total, core * each, each, 0)
    send_rows = lax.dynamic_slice_in_dim(total, (1 - core) * each, each, 0)
    got_rows = shift(send_rows, "c", 1)
    grad_mine = jnp.where(core == 0, keep_rows, got_rows)
    curve_mine = jnp.where(core == 0, got_rows, keep_rows)

    scaling = 1.0 / math.sqrt(tokens * 512)
    gradient = grad_mine * scaling
    curvature = curve_mine * scaling
    diag_est = my_probes.astype(jnp.float32) * curvature
    new_m = beta_one * m_old + (1.0 - beta_one) * gradient
    new_v = beta_two * v_old + (1.0 - beta_two) * diag_est * diag_est
    first_fix = 1.0 - beta_one**OPT_STEP
    second_fix = 1.0 - beta_two**OPT_STEP
    update = new_m / first_fix / (jnp.sqrt(new_v / second_fix) + epsilon)
    fresh = (own_rows.astype(jnp.float32) - learn_rate * update).astype(jnp.bfloat16)

    spread_rows = jnp.broadcast_to(fresh[None], (32, *fresh.shape))
    mine_rows = lax.all_to_all(spread_rows, ("yl", "z"), 0, 0, tiled=True)
    twin_rows = shift(mine_rows, "c", 1)
    both = jnp.stack(
        [jnp.where(core == 0, mine_rows, twin_rows), jnp.where(core == 0, twin_rows, mine_rows)], axis=1
    )
    new_w = both.reshape(w_out.shape)
    return (new_w, new_m, new_v)


def solution(mesh):
    fine = Mesh(mesh.devices.reshape(4, 8, 2, 2, 4), ("yl", "z", "c", "yh", "x"))
    dp, shard = ("yl", "z", "c"), ("yh", "x")
    return jax.shard_map(
        step,
        mesh=fine,
        in_specs=(
            P(dp + shard, None),
            P(shard, dp),
            P(shard, dp),
            P(shard, None),
            P(shard, None),
            P(shard + dp, None),
            P(shard + dp, None),
        ),
        out_specs=(P(shard, None), P(shard + dp, None), P(shard + dp, None)),
        check_vma=False,
    )
```

```python
import math

import jax
import jax.numpy as jnp
from jax import lax
from jax.sharding import Mesh, PartitionSpec as P


OPT_STEP = 10


beta_one = 0.9
beta_two = 0.999
learn_rate = 0.15
epsilon = 0.0001


def size(axis):
    return 8 if axis == "y" else lax.axis_size(axis)


def shift(value, axis, by):
    n = size(axis)
    hops = [(i, (i + by) % n) for i in range(n)]
    if axis == "y":
        at = [2 * (y % 4) + y // 4 for y in range(n)]
        return lax.ppermute(value, ("yl", "yh"), [(at[i], at[j]) for i, j in hops])
    return lax.ppermute(value, axis, hops)


def unpack_signs(signs):
    shifts = jnp.arange(32, dtype=jnp.int32)
    bit_values = jnp.bitwise_and(jnp.right_shift(signs[:, None, :], shifts[None, :, None]), 1)
    return (1 - 2 * bit_values).reshape(signs.shape[0] * 32, signs.shape[1]).astype(jnp.bfloat16)


def step(hidden, resid, target, w_out, signs, m_old, v_old):
    features, width = w_out.shape
    tokens = hidden.shape[0]
    group = tokens * lax.axis_size("x")
    half = lax.axis_index("yh")
    core = lax.axis_index("c")
    col = lax.axis_index("x")

    from_left = shift(hidden, "x", 1)
    from_right = shift(hidden, "x", -1)

    rows = features // 2
    part = shift(lax.dynamic_slice_in_dim(w_out, core * rows, rows, 0), "yh", 1)
    other_signs = shift(signs, "yh", 1)

    def gap(at):
        first = lax.dynamic_slice_in_dim(resid, at * group, group, 1)
        return first.astype(jnp.float32) - lax.dynamic_slice_in_dim(
            target, at * group, group, 1
        ).astype(jnp.float32)

    other_gap = shift(gap(1 - half).astype(jnp.bfloat16), "yh", 1)
    far_top = shift(from_left[: tokens // 2], "x", 1)
    far_low = shift(from_right[tokens // 2 :], "x", -1)
    twin = shift(part, "c", 1)

    def in_order(own, other):
        return jnp.concatenate(
            [jnp.where(half == 0, own, other), jnp.where(half == 0, other, own)], axis=0
        )

    probes = unpack_signs(signs)
    other_w = jnp.concatenate(
        [jnp.where(core == 0, part, twin), jnp.where(core == 0, twin, part)], axis=0
    )
    stacked = jnp.concatenate(
        [in_order(w_out, other_w), in_order(probes, unpack_signs(other_signs))], axis=0
    )
    gaps = in_order(gap(half), other_gap.astype(jnp.float32))
    gaps = jnp.concatenate([gaps, gaps], axis=1)
    count = 2 * features

    def run(block, first):
        here = lax.dynamic_slice_in_dim(gaps, ((col + first) % 4) * tokens, block.shape[0], 1)
        forward = lax.dot_general(
            stacked, block, (((1,), (1,)), ((), ())), preferred_element_type=jnp.float32
        )
        misfit = here + forward[:count]
        spread = 1.0 + misfit * misfit
        rooted = jnp.sqrt(spread)
        slopes = (misfit / rooted).astype(jnp.bfloat16)
        bends = (forward[count:] / (spread * rooted)).astype(jnp.bfloat16)
        away = jnp.where(core == 0, bends, slopes)
        kept = jnp.where(core == 0, slopes, bends)
        return away, kept

    def products(terms, block):
        return jnp.dot(terms, block, preferred_element_type=jnp.float32)

    near = jnp.concatenate([from_left, hidden, from_right], axis=0)
    away, kept = run(near, 3)
    away_near = products(away, near)
    kept_near = products(kept, near)
    away_near, kept_near, far_top, far_low = lax.optimization_barrier(
        (away_near, kept_near, far_top, far_low)
    )
    far = jnp.concatenate([far_top, far_low], axis=0)
    away, kept = run(far, 2)
    got = [
        shift(away_near[rows] + products(away[rows], far), "c", 1)
        for rows in (slice(0, features), slice(features, None))
    ]
    kept_all = kept_near + products(kept, far)
    mine = jnp.concatenate(
        [kept_all[:features] + got[0], kept_all[features:] + got[1]], axis=0
    ).astype(jnp.bfloat16)

    each = m_old.shape[0]
    row_start = (
        (lax.axis_index("yl") * lax.axis_size("z") + lax.axis_index("z")) * 2 + core
    ) * each
    my_probes = lax.dynamic_slice_in_dim(unpack_signs(signs).reshape(-1, 128), row_start, each, 0)
    own_rows = lax.dynamic_slice_in_dim(w_out.reshape(-1, 128), row_start, each, 0)
    plane = 64
    pieces = mine.reshape(plane, count * width // (plane * 128), 128)
    terms = lax.all_to_all(pieces, ("yh", "yl", "z"), 0, 0, tiled=True)
    terms, my_probes, own_rows = lax.optimization_barrier((terms, my_probes, own_rows))
    total = jnp.sum(terms.astype(jnp.float32), axis=0)
    keep_rows = lax.dynamic_slice_in_dim(total, core * each, each, 0)
    send_rows = lax.dynamic_slice_in_dim(total, (1 - core) * each, each, 0)
    got_rows = shift(send_rows, "c", 1)
    grad_mine = jnp.where(core == 0, keep_rows, got_rows)
    curve_mine = jnp.where(core == 0, got_rows, keep_rows)

    scaling = 1.0 / math.sqrt(tokens * 512)
    gradient = grad_mine * scaling
    curvature = curve_mine * scaling
    diag_est = my_probes.astype(jnp.float32) * curvature
    new_m = beta_one * m_old + (1.0 - beta_one) * gradient
    new_v = beta_two * v_old + (1.0 - beta_two) * diag_est * diag_est
    first_fix = 1.0 - beta_one**OPT_STEP
    second_fix = 1.0 - beta_two**OPT_STEP
    update = new_m / first_fix / (jnp.sqrt(new_v / second_fix) + epsilon)
    fresh = (own_rows.astype(jnp.float32) - learn_rate * update).astype(jnp.bfloat16)

    spread_rows = jnp.broadcast_to(fresh[None], (32, *fresh.shape))
    mine_rows = lax.all_to_all(spread_rows, ("yl", "z"), 0, 0, tiled=True)
    twin_rows = shift(mine_rows, "c", 1)
    both = jnp.stack(
        [jnp.where(core == 0, mine_rows, twin_rows), jnp.where(core == 0, twin_rows, mine_rows)], axis=1
    )
    new_w = both.reshape(w_out.shape)
    return (new_w, new_m, new_v)


def solution(mesh):
    fine = Mesh(mesh.devices.reshape(4, 8, 2, 2, 4), ("yl", "z", "c", "yh", "x"))
    dp, shard = ("yl", "z", "c"), ("yh", "x")
    return jax.shard_map(
        step,
        mesh=fine,
        in_specs=(
            P(dp + shard, None),
            P(shard, dp),
            P(shard, dp),
            P(shard, None),
            P(shard, None),
            P(shard + dp, None),
            P(shard + dp, None),
        ),
        out_specs=(P(shard, None), P(shard + dp, None), P(shard + dp, None)),
        check_vma=False,
    )
```

```python
import math

import jax
import jax.numpy as jnp
from jax import lax
from jax.experimental import pallas as pl
from jax.experimental.pallas import tpu as pltpu
from jax.sharding import Mesh, PartitionSpec as P


OPT_STEP = 10


beta_one = 0.9
beta_two = 0.999
learn_rate = 0.15
epsilon = 0.0001


def size(axis):
    return 8 if axis == "y" else lax.axis_size(axis)


def shift(value, axis, by):
    n = size(axis)
    hops = [(i, (i + by) % n) for i in range(n)]
    if axis == "y":
        at = [2 * (y % 4) + y // 4 for y in range(n)]
        return lax.ppermute(value, ("yl", "yh"), [(at[i], at[j]) for i, j in hops])
    return lax.ppermute(value, axis, hops)


def unpack_signs(signs):
    shifts = jnp.arange(32, dtype=jnp.int32)
    bit_values = jnp.bitwise_and(jnp.right_shift(signs[:, None, :], shifts[None, :, None]), 1)
    return (1 - 2 * bit_values).reshape(signs.shape[0] * 32, signs.shape[1]).astype(jnp.bfloat16)


def cut_kernel(half_ref, *refs):
    out_ref, lines = refs[6:]
    piece = out_ref.shape[1]
    per_row = refs[0].shape[1] // 128
    block = 8 * piece // per_row
    steps = refs[0].shape[0] // block

    for part in range(2):
        near_ref, far_ref, got_ref = refs[3 * part : 3 * part + 3]
        side = half_ref[0] if part == 0 else 1 - half_ref[0]

        @pl.loop(0, steps)
        def _(step):
            base = pl.multiple_of(step * block, 8)
            for group in range(0, block, 8):
                at = pl.ds(base + group, 8)
                rows = near_ref[at, :] + far_ref[at, :] + got_ref[at, :]
                for lane in range(per_row):
                    lines[pl.ds(group * per_row + lane, 8, stride=per_row), :] = rows[
                        :, lane * 128 : (lane + 1) * 128
                    ]
            for i in range(8):
                out_ref[(side * steps + step) * 8 + i] = lines[i * piece : (i + 1) * piece, :].astype(
                    jnp.bfloat16
                )


def cut(half, terms, plane):
    cells = 2 * terms[0].size
    piece = cells // (plane * 128)
    whole = pl.BlockSpec(memory_space=pltpu.VMEM)
    return pl.pallas_call(
        cut_kernel,
        out_shape=jax.ShapeDtypeStruct((plane, piece, 128), jnp.bfloat16),
        in_specs=[pl.BlockSpec(memory_space=pltpu.SMEM)] + [whole] * 6,
        out_specs=whole,
        scratch_shapes=[pltpu.VMEM((8 * piece, 128), jnp.float32)],
        compiler_params=pltpu.CompilerParams(vmem_limit_bytes=20 << 20),
        cost_estimate=pl.CostEstimate(flops=2 * cells, bytes_accessed=14 * cells, transcendentals=0),
        name="cut",
    )(half.reshape(1).astype(jnp.int32), *terms)


def step(hidden, resid, target, w_out, signs, m_old, v_old):
    features, _ = w_out.shape
    tokens = hidden.shape[0]
    group = tokens * lax.axis_size("x")
    half = lax.axis_index("yh")
    core = lax.axis_index("c")
    col = lax.axis_index("x")

    cutoff = tokens // 2
    top, low = hidden[:cutoff], hidden[cutoff:]
    left_top = shift(top, "x", 1)
    right_low = shift(low, "x", -1)
    left_low = shift(low, "x", 1)
    right_top = shift(top, "x", -1)
    far_top = shift(left_top, "x", 1)
    far_low = shift(right_low, "x", -1)

    rows = features // 2
    part = shift(lax.dynamic_slice_in_dim(w_out, core * rows, rows, 0), "yh", 1)
    other_signs = shift(signs, "yh", 1)

    def gap(at, kind):
        def part(whole):
            return lax.dynamic_slice_in_dim(whole, at * group, group, 1).astype(jnp.float32)

        gaps = (part(resid) - part(target)).astype(kind)
        gaps = jnp.concatenate([gaps, gaps], axis=1)
        return lax.dynamic_slice_in_dim(gaps, ((col + 3) % 4) * tokens, group, 1)

    other_gaps = shift(gap(1 - half, jnp.bfloat16), "yh", 1)
    twin = shift(part, "c", 1)
    probes = unpack_signs(signs)
    own_stack = jnp.concatenate([w_out, probes], axis=0)
    own_gaps = gap(half, jnp.float32)
    left_top, left_low, right_top, right_low, twin = lax.optimization_barrier(
        (left_top, left_low, right_top, right_low, twin)
    )
    other_signs, _ = lax.optimization_barrier((other_signs, probes))
    other_stack = jnp.concatenate(
        [
            jnp.where(core == 0, part, twin),
            jnp.where(core == 0, twin, part),
            unpack_signs(other_signs),
        ],
        axis=0,
    )

    def run(stacked, gaps, block):
        here = gaps[:, : block.shape[0]] if block.shape[0] > tokens else gaps[:, -tokens:]
        forward = lax.dot_general(
            stacked, block, (((1,), (1,)), ((), ())), preferred_element_type=jnp.float32
        )
        misfit = here.astype(jnp.float32) + forward[:features]
        spread = 1.0 + misfit * misfit
        rooted = jnp.sqrt(spread)
        slopes = (misfit / rooted).astype(jnp.bfloat16)
        bends = (forward[features:] / (spread * rooted)).astype(jnp.bfloat16)
        away = jnp.where(core == 0, bends, slopes)
        kept = jnp.where(core == 0, slopes, bends)
        return [jnp.dot(terms, block, preferred_element_type=jnp.float32) for terms in (away, kept)]

    near = jnp.concatenate([left_top, left_low, hidden, right_top, right_low], axis=0)
    own_away, own_kept = run(own_stack, own_gaps, near)
    other_away, other_kept = run(other_stack, other_gaps, near)
    own_away, own_kept, other_away, other_kept, far_top, far_low = lax.optimization_barrier(
        (own_away, own_kept, other_away, other_kept, far_top, far_low)
    )
    far = jnp.concatenate([far_top, far_low], axis=0)
    own_far = run(own_stack, own_gaps, far)
    own_got = shift(own_away + own_far[0], "c", 1)
    other_far = run(other_stack, other_gaps, far)
    other_got = shift(other_away + other_far[0], "c", 1)
    pieces = cut(half, (own_kept, own_far[1], own_got, other_kept, other_far[1], other_got), 64)

    each = m_old.shape[0]
    row_start = (
        (lax.axis_index("yl") * lax.axis_size("z") + lax.axis_index("z")) * 2 + core
    ) * each
    my_probes = lax.dynamic_slice_in_dim(unpack_signs(signs).reshape(-1, 128), row_start, each, 0)
    own_rows = lax.dynamic_slice_in_dim(w_out.reshape(-1, 128), row_start, each, 0)
    terms = lax.all_to_all(pieces, ("yh", "yl", "z"), 0, 0, tiled=True)
    terms, my_probes, own_rows = lax.optimization_barrier((terms, my_probes, own_rows))
    total = jnp.sum(terms.astype(jnp.float32), axis=0)
    keep_rows = lax.dynamic_slice_in_dim(total, core * each, each, 0)
    send_rows = lax.dynamic_slice_in_dim(total, (1 - core) * each, each, 0)
    got_rows = shift(send_rows, "c", 1)
    grad_mine = jnp.where(core == 0, keep_rows, got_rows)
    curve_mine = jnp.where(core == 0, got_rows, keep_rows)

    scaling = 1.0 / math.sqrt(tokens * 512)
    gradient = grad_mine * scaling
    curvature = curve_mine * scaling
    diag_est = my_probes.astype(jnp.float32) * curvature
    new_m = beta_one * m_old + (1.0 - beta_one) * gradient
    new_v = beta_two * v_old + (1.0 - beta_two) * diag_est * diag_est
    first_fix = 1.0 - beta_one**OPT_STEP
    second_fix = 1.0 - beta_two**OPT_STEP
    update = new_m / first_fix / (jnp.sqrt(new_v / second_fix) + epsilon)
    fresh = (own_rows.astype(jnp.float32) - learn_rate * update).astype(jnp.bfloat16)

    spread_rows = jnp.broadcast_to(fresh[None], (32, *fresh.shape))
    mine_rows = lax.all_to_all(spread_rows, ("yl", "z"), 0, 0, tiled=True)
    twin_rows = shift(mine_rows, "c", 1)
    both = jnp.stack([jnp.where(core == 0, mine_rows, twin_rows), jnp.where(core == 0, twin_rows, mine_rows)], axis=1)
    new_w = both.reshape(w_out.shape)
    return (new_w, new_m, new_v)


def solution(mesh):
    fine = Mesh(mesh.devices.reshape(4, 8, 2, 2, 4), ("yl", "z", "c", "yh", "x"))
    dp, shard = ("yl", "z", "c"), ("yh", "x")
    return jax.shard_map(
        step,
        mesh=fine,
        in_specs=(
            P(dp + shard, None),
            P(shard, dp),
            P(shard, dp),
            P(shard, None),
            P(shard, None),
            P(shard + dp, None),
            P(shard + dp, None),
        ),
        out_specs=(P(shard, None), P(shard + dp, None), P(shard + dp, None)),
        check_vma=False,
    )
```

```python
import math

import jax
import jax.numpy as jnp
from jax import lax
from jax.experimental import pallas as pl
from jax.experimental.pallas import tpu as pltpu
from jax.sharding import Mesh, PartitionSpec as P


OPT_STEP = 10


beta_one = 0.9
beta_two = 0.999
learn_rate = 0.15
epsilon = 0.0001


def size(axis):
    return 8 if axis == "y" else lax.axis_size(axis)


def shift(value, axis, by):
    n = size(axis)
    hops = [(i, (i + by) % n) for i in range(n)]
    if axis == "y":
        at = [2 * (y % 4) + y // 4 for y in range(n)]
        return lax.ppermute(value, ("yl", "yh"), [(at[i], at[j]) for i, j in hops])
    return lax.ppermute(value, axis, hops)


def unpack_signs(signs):
    shifts = jnp.arange(32, dtype=jnp.int32)
    bit_values = jnp.bitwise_and(jnp.right_shift(signs[:, None, :], shifts[None, :, None]), 1)
    return (1 - 2 * bit_values).reshape(signs.shape[0] * 32, signs.shape[1]).astype(jnp.bfloat16)


def cut_kernel(half_ref, *refs):
    out_ref, lines = refs[6:]
    piece = out_ref.shape[1]
    per_row = refs[0].shape[1] // 128
    block = 8 * piece // per_row
    steps = refs[0].shape[0] // block

    for part in range(2):
        near_ref, far_ref, got_ref = refs[3 * part : 3 * part + 3]
        side = half_ref[0] if part == 0 else 1 - half_ref[0]

        @pl.loop(0, steps)
        def _(step):
            base = pl.multiple_of(step * block, 8)
            for group in range(0, block, 8):
                at = pl.ds(base + group, 8)
                rows = near_ref[at, :] + far_ref[at, :] + got_ref[at, :]
                for lane in range(per_row):
                    lines[pl.ds(group * per_row + lane, 8, stride=per_row), :] = rows[
                        :, lane * 128 : (lane + 1) * 128
                    ]
            for i in range(8):
                out_ref[(side * steps + step) * 8 + i] = lines[i * piece : (i + 1) * piece, :].astype(
                    jnp.bfloat16
                )


def cut(half, terms, plane):
    cells = 2 * terms[0].size
    piece = cells // (plane * 128)
    whole = pl.BlockSpec(memory_space=pltpu.VMEM)
    return pl.pallas_call(
        cut_kernel,
        out_shape=jax.ShapeDtypeStruct((plane, piece, 128), jnp.bfloat16),
        in_specs=[pl.BlockSpec(memory_space=pltpu.SMEM)] + [whole] * 6,
        out_specs=whole,
        scratch_shapes=[pltpu.VMEM((8 * piece, 128), jnp.float32)],
        compiler_params=pltpu.CompilerParams(vmem_limit_bytes=20 << 20),
        cost_estimate=pl.CostEstimate(flops=2 * cells, bytes_accessed=14 * cells, transcendentals=0),
        name="cut",
    )(half.reshape(1).astype(jnp.int32), *terms)


def join_kernel(*refs):
    count = len(refs) - 2
    blocks, out_ref, arrived = refs[:count], refs[count], refs[count + 1]
    copies, at = [], 0
    for i, block in enumerate(blocks):
        size_here = block.shape[0]
        copies.append(
            pltpu.make_async_copy(block, out_ref.at[pl.ds(at, size_here), :], arrived.at[i])
        )
        copies[-1].start()
        at += size_here
    for copy in copies:
        copy.wait()


def join(blocks):
    rows, width = sum(b.shape[0] for b in blocks), blocks[0].shape[1]
    return pl.pallas_call(
        join_kernel,
        out_shape=jax.ShapeDtypeStruct((rows, width), blocks[0].dtype),
        in_specs=[pl.BlockSpec(memory_space=pl.ANY)] * len(blocks),
        out_specs=pl.BlockSpec(memory_space=pltpu.VMEM),
        scratch_shapes=[pltpu.SemaphoreType.DMA((len(blocks),))],
        compiler_params=pltpu.CompilerParams(vmem_limit_bytes=8 << 20),
        cost_estimate=pl.CostEstimate(
            flops=rows * width, bytes_accessed=4 * rows * width, transcendentals=0
        ),
        name="join",
    )(*blocks)


def step(hidden, resid, target, w_out, signs, m_old, v_old):
    features, width = w_out.shape
    tokens = hidden.shape[0]
    group = tokens * lax.axis_size("x")
    half = lax.axis_index("yh")
    core = lax.axis_index("c")
    col = lax.axis_index("x")

    cutoff = tokens // 2
    top, low = hidden[:cutoff], hidden[cutoff:]
    left_top = shift(top, "x", 1)
    right_low = shift(low, "x", -1)
    left_low = shift(low, "x", 1)
    right_top = shift(top, "x", -1)
    far_top = shift(left_top, "x", 1)
    far_low = shift(right_low, "x", -1)

    rows = features // 2
    octets = jnp.stack([(signs >> (16 * core + 8 * p)) & 255 for p in range(2)])
    part = jnp.concatenate(
        [
            lax.dynamic_slice_in_dim(w_out, core * rows, rows, 0),
            octets.reshape(-1, width).astype(jnp.bfloat16),
        ],
        axis=0,
    )
    part = shift(part, "yh", 1)

    def gap(at, kind):
        def part(whole):
            return lax.dynamic_slice_in_dim(whole, at * group, group, 1).astype(jnp.float32)

        gaps = (part(resid) - part(target)).astype(kind)
        gaps = jnp.concatenate([gaps, gaps], axis=1)
        return lax.dynamic_slice_in_dim(gaps, ((col + 3) % 4) * tokens, group, 1)

    other_gaps = shift(gap(1 - half, jnp.bfloat16), "yh", 1)
    twin = shift(part, "c", 1)
    probes = unpack_signs(signs)
    own_stack = jnp.concatenate([w_out, probes], axis=0)
    own_gaps = gap(half, jnp.float32)
    first = jnp.where(core == 0, part, twin)
    second = jnp.where(core == 0, twin, part)
    octets = jnp.stack([first[rows:], second[rows:]]).astype(jnp.int32)
    octets = octets.reshape(4, -1, 1, width).transpose(1, 0, 2, 3)
    bits = (octets >> jnp.arange(8, dtype=jnp.int32)[None, None, :, None]) & 1
    other_stack = jnp.concatenate(
        [first[:rows], second[:rows], (1 - 2 * bits).reshape(-1, width).astype(jnp.bfloat16)], axis=0
    )

    def run(stacked, gaps, block):
        here = gaps[:, : block.shape[0]] if block.shape[0] > tokens else gaps[:, -tokens:]
        forward = lax.dot_general(
            stacked, block, (((1,), (1,)), ((), ())), preferred_element_type=jnp.float32
        )
        misfit = here.astype(jnp.float32) + forward[:features]
        spread = 1.0 + misfit * misfit
        rooted = jnp.sqrt(spread)
        slopes = (misfit / rooted).astype(jnp.bfloat16)
        bends = (forward[features:] / (spread * rooted)).astype(jnp.bfloat16)
        away = jnp.where(core == 0, bends, slopes)
        kept = jnp.where(core == 0, slopes, bends)
        return [jnp.dot(terms, block, preferred_element_type=jnp.float32) for terms in (away, kept)]

    near = join((left_top, left_low, hidden, right_top, right_low))
    own_away, own_kept = run(own_stack, own_gaps, near)
    other_away, other_kept = run(other_stack, other_gaps, near)
    own_away, own_kept, other_away, other_kept, far_top, far_low = lax.optimization_barrier(
        (own_away, own_kept, other_away, other_kept, far_top, far_low)
    )
    far = join((far_top, far_low))
    own_far = run(own_stack, own_gaps, far)
    own_got = shift(own_away + own_far[0], "c", 1)
    other_far = run(other_stack, other_gaps, far)
    other_got = shift(other_away + other_far[0], "c", 1)
    pieces = cut(half, (own_kept, own_far[1], own_got, other_kept, other_far[1], other_got), 64)

    each = m_old.shape[0]
    row_start = (
        (lax.axis_index("yl") * lax.axis_size("z") + lax.axis_index("z")) * 2 + core
    ) * each
    my_probes = lax.dynamic_slice_in_dim(unpack_signs(signs).reshape(-1, 128), row_start, each, 0)
    own_rows = lax.dynamic_slice_in_dim(w_out.reshape(-1, 128), row_start, each, 0)
    terms = lax.all_to_all(pieces, ("yh", "yl", "z"), 0, 0, tiled=True)
    terms, my_probes, own_rows = lax.optimization_barrier((terms, my_probes, own_rows))
    total = jnp.sum(terms.astype(jnp.float32), axis=0)
    keep_rows = lax.dynamic_slice_in_dim(total, core * each, each, 0)
    send_rows = lax.dynamic_slice_in_dim(total, (1 - core) * each, each, 0)
    got_rows = shift(send_rows, "c", 1)
    grad_mine = jnp.where(core == 0, keep_rows, got_rows)
    curve_mine = jnp.where(core == 0, got_rows, keep_rows)

    scaling = 1.0 / math.sqrt(tokens * 512)
    gradient = grad_mine * scaling
    curvature = curve_mine * scaling
    diag_est = my_probes.astype(jnp.float32) * curvature
    new_m = beta_one * m_old + (1.0 - beta_one) * gradient
    new_v = beta_two * v_old + (1.0 - beta_two) * diag_est * diag_est
    first_fix = 1.0 - beta_one**OPT_STEP
    second_fix = 1.0 - beta_two**OPT_STEP
    update = new_m / first_fix / (jnp.sqrt(new_v / second_fix) + epsilon)
    fresh = (own_rows.astype(jnp.float32) - learn_rate * update).astype(jnp.bfloat16)

    spread_rows = jnp.broadcast_to(fresh[None], (32, *fresh.shape))
    mine_rows = lax.all_to_all(spread_rows, ("yl", "z"), 0, 0, tiled=True)
    twin_rows = shift(mine_rows, "c", 1)
    both = jnp.stack([jnp.where(core == 0, mine_rows, twin_rows), jnp.where(core == 0, twin_rows, mine_rows)], axis=1)
    new_w = both.reshape(w_out.shape)
    return (new_w, new_m, new_v)


def solution(mesh):
    fine = Mesh(mesh.devices.reshape(4, 8, 2, 2, 4), ("yl", "z", "c", "yh", "x"))
    dp, shard = ("yl", "z", "c"), ("yh", "x")
    return jax.shard_map(
        step,
        mesh=fine,
        in_specs=(
            P(dp + shard, None),
            P(shard, dp),
            P(shard, dp),
            P(shard, None),
            P(shard, None),
            P(shard + dp, None),
            P(shard + dp, None),
        ),
        out_specs=(P(shard, None), P(shard + dp, None), P(shard + dp, None)),
        check_vma=False,
    )
```

```python
import functools
import math

import jax
import jax.numpy as jnp
from jax import lax
from jax.experimental import pallas as pl
from jax.experimental.pallas import tpu as pltpu
from jax.sharding import Mesh, PartitionSpec as P


OPT_STEP = 10


beta_one = 0.9
beta_two = 0.999
learn_rate = 0.15
epsilon = 0.0001


def size(axis):
    return 8 if axis == "y" else lax.axis_size(axis)


def shift(value, axis, by):
    n = size(axis)
    hops = [(i, (i + by) % n) for i in range(n)]
    if axis == "y":
        at = [2 * (y % 4) + y // 4 for y in range(n)]
        return lax.ppermute(value, ("yl", "yh"), [(at[i], at[j]) for i, j in hops])
    return lax.ppermute(value, axis, hops)


def unpack_signs(signs):
    shifts = jnp.arange(32, dtype=jnp.int32)
    bit_values = jnp.bitwise_and(jnp.right_shift(signs[:, None, :], shifts[None, :, None]), 1)
    return (1 - 2 * bit_values).reshape(signs.shape[0] * 32, signs.shape[1]).astype(jnp.bfloat16)


def cut_kernel(half_ref, *refs):
    out_ref, lines = refs[6:]
    piece = out_ref.shape[1]
    per_row = refs[0].shape[1] // 128
    block = 8 * piece // per_row
    steps = refs[0].shape[0] // block

    for part in range(2):
        near_ref, far_ref, got_ref = refs[3 * part : 3 * part + 3]
        side = half_ref[0] if part == 0 else 1 - half_ref[0]

        @pl.loop(0, steps)
        def _(step):
            base = pl.multiple_of(step * block, 8)
            for group in range(0, block, 8):
                at = pl.ds(base + group, 8)
                rows = near_ref[at, :] + far_ref[at, :] + got_ref[at, :]
                for lane in range(per_row):
                    lines[pl.ds(group * per_row + lane, 8, stride=per_row), :] = rows[
                        :, lane * 128 : (lane + 1) * 128
                    ]
            for i in range(8):
                out_ref[(side * steps + step) * 8 + i] = lines[i * piece : (i + 1) * piece, :].astype(
                    jnp.bfloat16
                )


def cut(half, terms, plane):
    cells = 2 * terms[0].size
    piece = cells // (plane * 128)
    whole = pl.BlockSpec(memory_space=pltpu.VMEM)
    return pl.pallas_call(
        cut_kernel,
        out_shape=jax.ShapeDtypeStruct((plane, piece, 128), jnp.bfloat16),
        in_specs=[pl.BlockSpec(memory_space=pltpu.SMEM)] + [whole] * 6,
        out_specs=whole,
        scratch_shapes=[pltpu.VMEM((8 * piece, 128), jnp.float32)],
        compiler_params=pltpu.CompilerParams(vmem_limit_bytes=20 << 20),
        cost_estimate=pl.CostEstimate(flops=2 * cells, bytes_accessed=14 * cells, transcendentals=0),
        name="cut",
    )(half.reshape(1).astype(jnp.int32), *terms)


def pack_kernel(core_ref, weights_ref, signs_ref, out_ref):
    core, words = core_ref[0], signs_ref.shape[0]
    rows = out_ref.shape[0] - 2 * words
    out_ref[:rows, :] = weights_ref[pl.ds(pl.multiple_of(core * rows, 16), rows), :]
    for p in range(2):
        octet = jnp.right_shift(signs_ref[...], 16 * core + 8 * p) & 255
        out_ref[rows + p * words : rows + (p + 1) * words, :] = octet.astype(jnp.float32).astype(
            jnp.bfloat16
        )


def pack(core, weights, signs):
    rows = weights.shape[0] // 2 + 2 * signs.shape[0]
    whole = pl.BlockSpec(memory_space=pltpu.VMEM)
    return pl.pallas_call(
        pack_kernel,
        out_shape=jax.ShapeDtypeStruct((rows, weights.shape[1]), jnp.bfloat16),
        in_specs=[pl.BlockSpec(memory_space=pltpu.SMEM), whole, whole],
        out_specs=whole,
        compiler_params=pltpu.CompilerParams(vmem_limit_bytes=4 << 20),
        cost_estimate=pl.CostEstimate(
            flops=weights.size, bytes_accessed=2 * weights.size, transcendentals=0
        ),
        name="pack",
    )(core.reshape(1).astype(jnp.int32), weights, signs)


def unpack_kernel(words, core_ref, part_ref, twin_ref, out_ref):
    first = core_ref[0] == 0
    rows = part_ref.shape[0] - 2 * words
    width = part_ref.shape[1]

    def fill(low_ref, high_ref):
        out_ref[:rows, :] = low_ref[:rows, :]
        out_ref[rows : 2 * rows, :] = high_ref[:rows, :]
        place_in_byte = lax.broadcasted_iota(jnp.int32, (8, width), 0)
        for k in range(words):
            for q, source in enumerate((low_ref, high_ref)):
                signs = []
                for p in range(2):
                    at = rows + p * words + k
                    octet = source[at : at + 1, :].astype(jnp.float32).astype(jnp.int32)
                    bits = jnp.right_shift(jnp.broadcast_to(octet, (8, width)), place_in_byte) & 1
                    signs.append((1 - 2 * bits).astype(jnp.float32))
                base = 2 * rows + 32 * k + 16 * q
                out_ref[base : base + 16, :] = jnp.concatenate(signs, axis=0).astype(jnp.bfloat16)

    @pl.when(first)
    def _():
        fill(part_ref, twin_ref)

    @pl.when(jnp.logical_not(first))
    def _():
        fill(twin_ref, part_ref)


def unpack(core, part, twin, words):
    rows = 2 * (part.shape[0] - 2 * words) + 32 * words
    whole = pl.BlockSpec(memory_space=pltpu.VMEM)
    return pl.pallas_call(
        functools.partial(unpack_kernel, words),
        out_shape=jax.ShapeDtypeStruct((rows, part.shape[1]), jnp.bfloat16),
        in_specs=[pl.BlockSpec(memory_space=pltpu.SMEM), whole, whole],
        out_specs=whole,
        compiler_params=pltpu.CompilerParams(vmem_limit_bytes=6 << 20),
        cost_estimate=pl.CostEstimate(
            flops=8 * part.size, bytes_accessed=6 * part.size, transcendentals=0
        ),
        name="unpack",
    )(core.reshape(1).astype(jnp.int32), part, twin)


def join_kernel(*refs):
    count = len(refs) - 2
    blocks, out_ref, arrived = refs[:count], refs[count], refs[count + 1]
    copies, at = [], 0
    for i, block in enumerate(blocks):
        size_here = block.shape[0]
        copies.append(
            pltpu.make_async_copy(block, out_ref.at[pl.ds(at, size_here), :], arrived.at[i])
        )
        copies[-1].start()
        at += size_here
    for copy in copies:
        copy.wait()


def join(blocks):
    rows, width = sum(b.shape[0] for b in blocks), blocks[0].shape[1]
    return pl.pallas_call(
        join_kernel,
        out_shape=jax.ShapeDtypeStruct((rows, width), blocks[0].dtype),
        in_specs=[pl.BlockSpec(memory_space=pl.ANY)] * len(blocks),
        out_specs=pl.BlockSpec(memory_space=pltpu.VMEM),
        scratch_shapes=[pltpu.SemaphoreType.DMA((len(blocks),))],
        compiler_params=pltpu.CompilerParams(vmem_limit_bytes=8 << 20),
        cost_estimate=pl.CostEstimate(
            flops=rows * width, bytes_accessed=4 * rows * width, transcendentals=0
        ),
        name="join",
    )(*blocks)


def step(hidden, resid, target, w_out, signs, m_old, v_old):
    features, _ = w_out.shape
    tokens = hidden.shape[0]
    group = tokens * lax.axis_size("x")
    half = lax.axis_index("yh")
    core = lax.axis_index("c")
    col = lax.axis_index("x")

    cutoff = tokens // 2
    top, low = hidden[:cutoff], hidden[cutoff:]
    left_top = shift(top, "x", 1)
    right_low = shift(low, "x", -1)
    left_low = shift(low, "x", 1)
    right_top = shift(top, "x", -1)
    far_top = shift(left_top, "x", 1)
    far_low = shift(right_low, "x", -1)

    part = shift(pack(core, w_out, signs), "yh", 1)

    def gap(at, kind):
        def part(whole):
            return lax.dynamic_slice_in_dim(whole, at * group, group, 1).astype(jnp.float32)

        gaps = (part(resid) - part(target)).astype(kind)
        gaps = jnp.concatenate([gaps, gaps], axis=1)
        return lax.dynamic_slice_in_dim(gaps, ((col + 3) % 4) * tokens, group, 1)

    other_gaps = shift(gap(1 - half, jnp.bfloat16), "yh", 1)
    twin = shift(part, "c", 1)
    probes = unpack_signs(signs)
    own_stack = jnp.concatenate([w_out, probes], axis=0)
    own_gaps = gap(half, jnp.float32)
    other_stack = unpack(core, part, twin, signs.shape[0])

    def run(stacked, gaps, block):
        here = gaps[:, : block.shape[0]] if block.shape[0] > tokens else gaps[:, -tokens:]
        forward = lax.dot_general(
            stacked, block, (((1,), (1,)), ((), ())), preferred_element_type=jnp.float32
        )
        misfit = here.astype(jnp.float32) + forward[:features]
        spread = 1.0 + misfit * misfit
        rooted = jnp.sqrt(spread)
        slopes = (misfit / rooted).astype(jnp.bfloat16)
        bends = (forward[features:] / (spread * rooted)).astype(jnp.bfloat16)
        away = jnp.where(core == 0, bends, slopes)
        kept = jnp.where(core == 0, slopes, bends)
        return [jnp.dot(terms, block, preferred_element_type=jnp.float32) for terms in (away, kept)]

    near = join((left_top, left_low, hidden, right_top, right_low))
    own_away, own_kept = run(own_stack, own_gaps, near)
    other_away, other_kept = run(other_stack, other_gaps, near)
    own_away, own_kept, other_away, other_kept, far_top, far_low = lax.optimization_barrier(
        (own_away, own_kept, other_away, other_kept, far_top, far_low)
    )
    far = join((far_top, far_low))
    own_far = run(own_stack, own_gaps, far)
    own_got = shift(own_away + own_far[0], "c", 1)
    other_far = run(other_stack, other_gaps, far)
    other_got = shift(other_away + other_far[0], "c", 1)
    pieces = cut(half, (own_kept, own_far[1], own_got, other_kept, other_far[1], other_got), 64)

    each = m_old.shape[0]
    row_start = (
        (lax.axis_index("yl") * lax.axis_size("z") + lax.axis_index("z")) * 2 + core
    ) * each
    my_probes = lax.dynamic_slice_in_dim(unpack_signs(signs).reshape(-1, 128), row_start, each, 0)
    own_rows = lax.dynamic_slice_in_dim(w_out.reshape(-1, 128), row_start, each, 0)
    terms = lax.all_to_all(pieces, ("yh", "yl", "z"), 0, 0, tiled=True)
    terms, my_probes, own_rows = lax.optimization_barrier((terms, my_probes, own_rows))
    total = jnp.sum(terms.astype(jnp.float32), axis=0)
    keep_rows = lax.dynamic_slice_in_dim(total, core * each, each, 0)
    send_rows = lax.dynamic_slice_in_dim(total, (1 - core) * each, each, 0)
    got_rows = shift(send_rows, "c", 1)
    grad_mine = jnp.where(core == 0, keep_rows, got_rows)
    curve_mine = jnp.where(core == 0, got_rows, keep_rows)

    scaling = 1.0 / math.sqrt(tokens * 512)
    gradient = grad_mine * scaling
    curvature = curve_mine * scaling
    diag_est = my_probes.astype(jnp.float32) * curvature
    new_m = beta_one * m_old + (1.0 - beta_one) * gradient
    new_v = beta_two * v_old + (1.0 - beta_two) * diag_est * diag_est
    first_fix = 1.0 - beta_one**OPT_STEP
    second_fix = 1.0 - beta_two**OPT_STEP
    update = new_m / first_fix / (jnp.sqrt(new_v / second_fix) + epsilon)
    fresh = (own_rows.astype(jnp.float32) - learn_rate * update).astype(jnp.bfloat16)

    spread_rows = jnp.broadcast_to(fresh[None], (32, *fresh.shape))
    mine_rows = lax.all_to_all(spread_rows, ("yl", "z"), 0, 0, tiled=True)
    twin_rows = shift(mine_rows, "c", 1)
    both = jnp.stack(
        [jnp.where(core == 0, mine_rows, twin_rows), jnp.where(core == 0, twin_rows, mine_rows)], axis=1
    )
    new_w = both.reshape(w_out.shape)
    return (new_w, new_m, new_v)


def solution(mesh):
    fine = Mesh(mesh.devices.reshape(4, 8, 2, 2, 4), ("yl", "z", "c", "yh", "x"))
    dp, shard = ("yl", "z", "c"), ("yh", "x")
    return jax.shard_map(
        step,
        mesh=fine,
        in_specs=(
            P(dp + shard, None),
            P(shard, dp),
            P(shard, dp),
            P(shard, None),
            P(shard, None),
            P(shard + dp, None),
            P(shard + dp, None),
        ),
        out_specs=(P(shard, None), P(shard + dp, None), P(shard + dp, None)),
        check_vma=False,
    )
```

```python
import functools
import math

import jax
import jax.numpy as jnp
from jax import lax
from jax.experimental import pallas as pl
from jax.experimental.pallas import tpu as pltpu
from jax.sharding import Mesh, PartitionSpec as P


OPT_STEP = 10


beta_one = 0.9
beta_two = 0.999
learn_rate = 0.15
epsilon = 0.0001


def size(axis):
    return 8 if axis == "y" else lax.axis_size(axis)


def shift(value, axis, by):
    n = size(axis)
    hops = [(i, (i + by) % n) for i in range(n)]
    if axis == "y":
        at = [2 * (y % 4) + y // 4 for y in range(n)]
        return lax.ppermute(value, ("yl", "yh"), [(at[i], at[j]) for i, j in hops])
    return lax.ppermute(value, axis, hops)


def unpack_signs(signs):
    shifts = jnp.arange(32, dtype=jnp.int32)
    bit_values = jnp.bitwise_and(jnp.right_shift(signs[:, None, :], shifts[None, :, None]), 1)
    return (1 - 2 * bit_values).reshape(signs.shape[0] * 32, signs.shape[1]).astype(jnp.bfloat16)


def cut_kernel(half_ref, *refs):
    out_ref, lines = refs[6:]
    piece = out_ref.shape[1]
    per_row = refs[0].shape[1] // 128
    block = 8 * piece // per_row
    steps = refs[0].shape[0] // block

    for part in range(2):
        near_ref, far_ref, got_ref = refs[3 * part : 3 * part + 3]
        side = half_ref[0] if part == 0 else 1 - half_ref[0]

        @pl.loop(0, steps)
        def _(step):
            base = pl.multiple_of(step * block, 8)
            for group in range(0, block, 8):
                at = pl.ds(base + group, 8)
                rows = near_ref[at, :] + far_ref[at, :] + got_ref[at, :]
                for lane in range(per_row):
                    lines[pl.ds(group * per_row + lane, 8, stride=per_row), :] = rows[
                        :, lane * 128 : (lane + 1) * 128
                    ]
            for i in range(8):
                out_ref[(side * steps + step) * 8 + i] = lines[i * piece : (i + 1) * piece, :].astype(
                    jnp.bfloat16
                )


def cut(half, terms, plane):
    cells = 2 * terms[0].size
    piece = cells // (plane * 128)
    whole = pl.BlockSpec(memory_space=pltpu.VMEM)
    return pl.pallas_call(
        cut_kernel,
        out_shape=jax.ShapeDtypeStruct((plane, piece, 128), jnp.bfloat16),
        in_specs=[pl.BlockSpec(memory_space=pltpu.SMEM)] + [whole] * 6,
        out_specs=whole,
        scratch_shapes=[pltpu.VMEM((8 * piece, 128), jnp.float32)],
        compiler_params=pltpu.CompilerParams(vmem_limit_bytes=20 << 20),
        cost_estimate=pl.CostEstimate(flops=2 * cells, bytes_accessed=14 * cells, transcendentals=0),
        name="cut",
    )(half.reshape(1).astype(jnp.int32), *terms)


def pack_kernel(core_ref, weights_ref, signs_ref, out_ref):
    core, words = core_ref[0], signs_ref.shape[0]
    rows = out_ref.shape[0] - 2 * words
    out_ref[:rows, :] = weights_ref[pl.ds(pl.multiple_of(core * rows, 16), rows), :]
    for p in range(2):
        octet = jnp.right_shift(signs_ref[...], 16 * core + 8 * p) & 255
        out_ref[rows + p * words : rows + (p + 1) * words, :] = octet.astype(jnp.float32).astype(
            jnp.bfloat16
        )


def pack(core, weights, signs):
    rows = weights.shape[0] // 2 + 2 * signs.shape[0]
    whole = pl.BlockSpec(memory_space=pltpu.VMEM)
    return pl.pallas_call(
        pack_kernel,
        out_shape=jax.ShapeDtypeStruct((rows, weights.shape[1]), jnp.bfloat16),
        in_specs=[pl.BlockSpec(memory_space=pltpu.SMEM), whole, whole],
        out_specs=whole,
        compiler_params=pltpu.CompilerParams(vmem_limit_bytes=4 << 20),
        cost_estimate=pl.CostEstimate(
            flops=weights.size, bytes_accessed=2 * weights.size, transcendentals=0
        ),
        name="pack",
    )(core.reshape(1).astype(jnp.int32), weights, signs)


def unpack_kernel(words, core_ref, part_ref, twin_ref, out_ref):
    first = core_ref[0] == 0
    rows = part_ref.shape[0] - 2 * words
    width = part_ref.shape[1]

    def fill(low_ref, high_ref):
        out_ref[:rows, :] = low_ref[:rows, :]
        out_ref[rows : 2 * rows, :] = high_ref[:rows, :]
        place_in_byte = lax.broadcasted_iota(jnp.int32, (8, width), 0)
        for k in range(words):
            for q, source in enumerate((low_ref, high_ref)):
                signs = []
                for p in range(2):
                    at = rows + p * words + k
                    octet = source[at : at + 1, :].astype(jnp.float32).astype(jnp.int32)
                    bits = jnp.right_shift(jnp.broadcast_to(octet, (8, width)), place_in_byte) & 1
                    signs.append((1 - 2 * bits).astype(jnp.float32))
                base = 2 * rows + 32 * k + 16 * q
                out_ref[base : base + 16, :] = jnp.concatenate(signs, axis=0).astype(jnp.bfloat16)

    @pl.when(first)
    def _():
        fill(part_ref, twin_ref)

    @pl.when(jnp.logical_not(first))
    def _():
        fill(twin_ref, part_ref)


def unpack(core, part, twin, words):
    rows = 2 * (part.shape[0] - 2 * words) + 32 * words
    whole = pl.BlockSpec(memory_space=pltpu.VMEM)
    return pl.pallas_call(
        functools.partial(unpack_kernel, words),
        out_shape=jax.ShapeDtypeStruct((rows, part.shape[1]), jnp.bfloat16),
        in_specs=[pl.BlockSpec(memory_space=pltpu.SMEM), whole, whole],
        out_specs=whole,
        compiler_params=pltpu.CompilerParams(vmem_limit_bytes=6 << 20),
        cost_estimate=pl.CostEstimate(
            flops=8 * part.size, bytes_accessed=6 * part.size, transcendentals=0
        ),
        name="unpack",
    )(core.reshape(1).astype(jnp.int32), part, twin)


def gap_kernel(spot_ref, resid_ref, target_ref, own_ref, other_ref):
    half, col = spot_ref[0], spot_ref[1]
    tokens = own_ref.shape[1] // 4
    for at, out_ref in ((half, own_ref), (1 - half, other_ref)):
        for j in range(4):
            start = at * 4 * tokens + lax.rem(col + 3 + j, 4) * tokens
            cols = pl.ds(pl.multiple_of(start, 128), tokens)
            gaps = resid_ref[:, cols].astype(jnp.float32) - target_ref[:, cols].astype(jnp.float32)
            out_ref[:, j * tokens : (j + 1) * tokens] = gaps.astype(out_ref.dtype)


def gap_pair(half, col, resid, target, group):
    whole = pl.BlockSpec(memory_space=pltpu.VMEM)
    shape = (resid.shape[0], group)
    return pl.pallas_call(
        gap_kernel,
        out_shape=[jax.ShapeDtypeStruct(shape, kind) for kind in (jnp.float32, jnp.bfloat16)],
        in_specs=[pl.BlockSpec(memory_space=pltpu.SMEM), whole, whole],
        out_specs=[whole, whole],
        compiler_params=pltpu.CompilerParams(vmem_limit_bytes=6 << 20),
        cost_estimate=pl.CostEstimate(
            flops=resid.size, bytes_accessed=8 * resid.size, transcendentals=0
        ),
        name="gap",
    )(jnp.stack([half, col]).astype(jnp.int32), resid, target)


def join_kernel(*refs):
    count = len(refs) - 2
    blocks, out_ref, arrived = refs[:count], refs[count], refs[count + 1]
    copies, at = [], 0
    for i, block in enumerate(blocks):
        size_here = block.shape[0]
        copies.append(
            pltpu.make_async_copy(block, out_ref.at[pl.ds(at, size_here), :], arrived.at[i])
        )
        copies[-1].start()
        at += size_here
    for copy in copies:
        copy.wait()


def join(blocks):
    rows, width = sum(b.shape[0] for b in blocks), blocks[0].shape[1]
    return pl.pallas_call(
        join_kernel,
        out_shape=jax.ShapeDtypeStruct((rows, width), blocks[0].dtype),
        in_specs=[pl.BlockSpec(memory_space=pl.ANY)] * len(blocks),
        out_specs=pl.BlockSpec(memory_space=pltpu.VMEM),
        scratch_shapes=[pltpu.SemaphoreType.DMA((len(blocks),))],
        compiler_params=pltpu.CompilerParams(vmem_limit_bytes=8 << 20),
        cost_estimate=pl.CostEstimate(
            flops=rows * width, bytes_accessed=4 * rows * width, transcendentals=0
        ),
        name="join",
    )(*blocks)


def step(hidden, resid, target, w_out, signs, m_old, v_old):
    features, _ = w_out.shape
    tokens = hidden.shape[0]
    group = tokens * lax.axis_size("x")
    half = lax.axis_index("yh")
    core = lax.axis_index("c")
    col = lax.axis_index("x")

    cutoff = tokens // 2
    top, low = hidden[:cutoff], hidden[cutoff:]
    left_top = shift(top, "x", 1)
    right_low = shift(low, "x", -1)
    left_low = shift(low, "x", 1)
    right_top = shift(top, "x", -1)
    far_top = shift(left_top, "x", 1)
    far_low = shift(right_low, "x", -1)

    part = shift(pack(core, w_out, signs), "yh", 1)

    own_gaps, other_gaps = gap_pair(half, col, resid, target, group)
    other_gaps = shift(other_gaps, "yh", 1)
    twin = shift(part, "c", 1)
    probes = unpack_signs(signs)
    own_stack = jnp.concatenate([w_out, probes], axis=0)
    other_stack = unpack(core, part, twin, signs.shape[0])

    def run(stacked, gaps, block):
        here = gaps[:, : block.shape[0]] if block.shape[0] > tokens else gaps[:, -tokens:]
        forward = lax.dot_general(
            stacked, block, (((1,), (1,)), ((), ())), preferred_element_type=jnp.float32
        )
        misfit = here.astype(jnp.float32) + forward[:features]
        spread = 1.0 + misfit * misfit
        rooted = jnp.sqrt(spread)
        slopes = (misfit / rooted).astype(jnp.bfloat16)
        bends = (forward[features:] / (spread * rooted)).astype(jnp.bfloat16)
        away = jnp.where(core == 0, bends, slopes)
        kept = jnp.where(core == 0, slopes, bends)
        away, kept = lax.optimization_barrier((away, kept))
        return [jnp.dot(terms, block, preferred_element_type=jnp.float32) for terms in (away, kept)]

    near = join((left_top, left_low, hidden, right_top, right_low))
    own_away, own_kept = run(own_stack, own_gaps, near)
    other_away, other_kept = run(other_stack, other_gaps, near)
    own_away, own_kept, other_away, other_kept, far_top, far_low = lax.optimization_barrier(
        (own_away, own_kept, other_away, other_kept, far_top, far_low)
    )
    far = join((far_top, far_low))
    own_far = run(own_stack, own_gaps, far)
    own_got = shift(own_away + own_far[0], "c", 1)
    other_far = run(other_stack, other_gaps, far)
    other_got = shift(other_away + other_far[0], "c", 1)
    pieces = cut(half, (own_kept, own_far[1], own_got, other_kept, other_far[1], other_got), 64)

    each = m_old.shape[0]
    row_start = (
        (lax.axis_index("yl") * lax.axis_size("z") + lax.axis_index("z")) * 2 + core
    ) * each
    my_probes = lax.dynamic_slice_in_dim(unpack_signs(signs).reshape(-1, 128), row_start, each, 0)
    own_rows = lax.dynamic_slice_in_dim(w_out.reshape(-1, 128), row_start, each, 0)
    terms = lax.all_to_all(pieces, ("yh", "yl", "z"), 0, 0, tiled=True)
    terms, my_probes, own_rows = lax.optimization_barrier((terms, my_probes, own_rows))
    total = jnp.sum(terms.astype(jnp.float32), axis=0)
    keep_rows = lax.dynamic_slice_in_dim(total, core * each, each, 0)
    send_rows = lax.dynamic_slice_in_dim(total, (1 - core) * each, each, 0)
    got_rows = shift(send_rows, "c", 1)
    grad_mine = jnp.where(core == 0, keep_rows, got_rows)
    curve_mine = jnp.where(core == 0, got_rows, keep_rows)

    scaling = 1.0 / math.sqrt(tokens * 512)
    gradient = grad_mine * scaling
    curvature = curve_mine * scaling
    diag_est = my_probes.astype(jnp.float32) * curvature
    new_m = beta_one * m_old + (1.0 - beta_one) * gradient
    new_v = beta_two * v_old + (1.0 - beta_two) * diag_est * diag_est
    first_fix = 1.0 - beta_one**OPT_STEP
    second_fix = 1.0 - beta_two**OPT_STEP
    update = new_m / first_fix / (jnp.sqrt(new_v / second_fix) + epsilon)
    fresh = (own_rows.astype(jnp.float32) - learn_rate * update).astype(jnp.bfloat16)

    spread_rows = jnp.broadcast_to(fresh[None], (32, *fresh.shape))
    mine_rows = lax.all_to_all(spread_rows, ("yl", "z"), 0, 0, tiled=True)
    twin_rows = shift(mine_rows, "c", 1)
    both = jnp.stack(
        [jnp.where(core == 0, mine_rows, twin_rows), jnp.where(core == 0, twin_rows, mine_rows)], axis=1
    )
    new_w = both.reshape(w_out.shape)
    return (new_w, new_m, new_v)


def solution(mesh):
    fine = Mesh(mesh.devices.reshape(4, 8, 2, 2, 4), ("yl", "z", "c", "yh", "x"))
    dp, shard = ("yl", "z", "c"), ("yh", "x")
    return jax.shard_map(
        step,
        mesh=fine,
        in_specs=(
            P(dp + shard, None),
            P(shard, dp),
            P(shard, dp),
            P(shard, None),
            P(shard, None),
            P(shard + dp, None),
            P(shard + dp, None),
        ),
        out_specs=(P(shard, None), P(shard + dp, None), P(shard + dp, None)),
        check_vma=False,
    )
```

```python
import functools
import math

import jax
import jax.numpy as jnp
from jax import lax
from jax.experimental import pallas as pl
from jax.experimental.pallas import tpu as pltpu
from jax.sharding import Mesh, PartitionSpec as P


OPT_STEP = 10


beta_one = 0.9
beta_two = 0.999
learn_rate = 0.15
epsilon = 0.0001


def size(axis):
    return 8 if axis == "y" else lax.axis_size(axis)


def shift(value, axis, by):
    n = size(axis)
    hops = [(i, (i + by) % n) for i in range(n)]
    if axis == "y":
        at = [2 * (y % 4) + y // 4 for y in range(n)]
        return lax.ppermute(value, ("yl", "yh"), [(at[i], at[j]) for i, j in hops])
    return lax.ppermute(value, axis, hops)


def unpack_signs(signs):
    shifts = jnp.arange(32, dtype=jnp.int32)
    bit_values = jnp.bitwise_and(jnp.right_shift(signs[:, None, :], shifts[None, :, None]), 1)
    return (1 - 2 * bit_values).reshape(signs.shape[0] * 32, signs.shape[1]).astype(jnp.bfloat16)


def cut_kernel(half_ref, *refs):
    out_ref, lines = refs[6:]
    piece = out_ref.shape[1]
    per_row = refs[0].shape[1] // 128
    block = 8 * piece // per_row
    steps = refs[0].shape[0] // block

    for part in range(2):
        near_ref, far_ref, got_ref = refs[3 * part : 3 * part + 3]
        side = half_ref[0] if part == 0 else 1 - half_ref[0]

        @pl.loop(0, steps)
        def _(step):
            base = pl.multiple_of(step * block, 8)
            for group in range(0, block, 8):
                at = pl.ds(base + group, 8)
                rows = near_ref[at, :] + far_ref[at, :] + got_ref[at, :]
                for lane in range(per_row):
                    lines[pl.ds(group * per_row + lane, 8, stride=per_row), :] = rows[
                        :, lane * 128 : (lane + 1) * 128
                    ]
            for i in range(8):
                out_ref[(side * steps + step) * 8 + i] = lines[i * piece : (i + 1) * piece, :].astype(
                    jnp.bfloat16
                )


def cut(half, terms, plane):
    cells = 2 * terms[0].size
    piece = cells // (plane * 128)
    whole = pl.BlockSpec(memory_space=pltpu.VMEM)
    return pl.pallas_call(
        cut_kernel,
        out_shape=jax.ShapeDtypeStruct((plane, piece, 128), jnp.bfloat16),
        in_specs=[pl.BlockSpec(memory_space=pltpu.SMEM)] + [whole] * 6,
        out_specs=whole,
        scratch_shapes=[pltpu.VMEM((8 * piece, 128), jnp.float32)],
        compiler_params=pltpu.CompilerParams(vmem_limit_bytes=20 << 20),
        cost_estimate=pl.CostEstimate(flops=2 * cells, bytes_accessed=14 * cells, transcendentals=0),
        name="cut",
    )(half.reshape(1).astype(jnp.int32), *terms)


def pack_kernel(core_ref, weights_ref, signs_ref, out_ref):
    core, words = core_ref[0], signs_ref.shape[0]
    rows = out_ref.shape[0] - 2 * words
    out_ref[:rows, :] = weights_ref[pl.ds(pl.multiple_of(core * rows, 16), rows), :]
    for p in range(2):
        octet = jnp.right_shift(signs_ref[...], 16 * core + 8 * p) & 255
        out_ref[rows + p * words : rows + (p + 1) * words, :] = octet.astype(jnp.float32).astype(
            jnp.bfloat16
        )


def pack(core, weights, signs):
    rows = weights.shape[0] // 2 + 2 * signs.shape[0]
    whole = pl.BlockSpec(memory_space=pltpu.VMEM)
    return pl.pallas_call(
        pack_kernel,
        out_shape=jax.ShapeDtypeStruct((rows, weights.shape[1]), jnp.bfloat16),
        in_specs=[pl.BlockSpec(memory_space=pltpu.SMEM), whole, whole],
        out_specs=whole,
        compiler_params=pltpu.CompilerParams(vmem_limit_bytes=4 << 20),
        cost_estimate=pl.CostEstimate(
            flops=weights.size, bytes_accessed=2 * weights.size, transcendentals=0
        ),
        name="pack",
    )(core.reshape(1).astype(jnp.int32), weights, signs)


def unpack_kernel(words, core_ref, part_ref, twin_ref, out_ref):
    first = core_ref[0] == 0
    rows = part_ref.shape[0] - 2 * words
    width = part_ref.shape[1]

    def fill(low_ref, high_ref):
        out_ref[:rows, :] = low_ref[:rows, :]
        out_ref[rows : 2 * rows, :] = high_ref[:rows, :]
        place_in_byte = lax.broadcasted_iota(jnp.int32, (8, width), 0)
        for k in range(words):
            for q, source in enumerate((low_ref, high_ref)):
                signs = []
                for p in range(2):
                    at = rows + p * words + k
                    octet = source[at : at + 1, :].astype(jnp.float32).astype(jnp.int32)
                    bits = jnp.right_shift(jnp.broadcast_to(octet, (8, width)), place_in_byte) & 1
                    signs.append((1 - 2 * bits).astype(jnp.float32))
                base = 2 * rows + 32 * k + 16 * q
                out_ref[base : base + 16, :] = jnp.concatenate(signs, axis=0).astype(jnp.bfloat16)

    @pl.when(first)
    def _():
        fill(part_ref, twin_ref)

    @pl.when(jnp.logical_not(first))
    def _():
        fill(twin_ref, part_ref)


def unpack(core, part, twin, words):
    rows = 2 * (part.shape[0] - 2 * words) + 32 * words
    whole = pl.BlockSpec(memory_space=pltpu.VMEM)
    return pl.pallas_call(
        functools.partial(unpack_kernel, words),
        out_shape=jax.ShapeDtypeStruct((rows, part.shape[1]), jnp.bfloat16),
        in_specs=[pl.BlockSpec(memory_space=pltpu.SMEM), whole, whole],
        out_specs=whole,
        compiler_params=pltpu.CompilerParams(vmem_limit_bytes=6 << 20),
        cost_estimate=pl.CostEstimate(
            flops=8 * part.size, bytes_accessed=6 * part.size, transcendentals=0
        ),
        name="unpack",
    )(core.reshape(1).astype(jnp.int32), part, twin)


def gap_kernel(spot_ref, resid_ref, target_ref, out_ref):
    base, col = spot_ref[0], spot_ref[1]
    tokens = out_ref.shape[1] // 4
    for j in range(4):
        cols = pl.ds(pl.multiple_of(base + lax.rem(col + 3 + j, 4) * tokens, 128), tokens)
        gaps = resid_ref[:, cols].astype(jnp.float32) - target_ref[:, cols].astype(jnp.float32)
        out_ref[:, j * tokens : (j + 1) * tokens] = gaps.astype(out_ref.dtype)


def gap(base, col, resid, target, group, kind):
    whole = pl.BlockSpec(memory_space=pltpu.VMEM)
    return pl.pallas_call(
        gap_kernel,
        out_shape=jax.ShapeDtypeStruct((resid.shape[0], group), kind),
        in_specs=[pl.BlockSpec(memory_space=pltpu.SMEM), whole, whole],
        out_specs=whole,
        compiler_params=pltpu.CompilerParams(vmem_limit_bytes=6 << 20),
        cost_estimate=pl.CostEstimate(
            flops=resid.size, bytes_accessed=6 * resid.size, transcendentals=0
        ),
        name="gap",
    )(jnp.stack([base, col]).astype(jnp.int32), resid, target)


def lay_kernel(core_ref, mine_ref, twin_ref, out_ref, lines):
    piece = mine_ref.shape[1]
    per_row = out_ref.shape[1] // 128
    block = 8
    rows = block * 2 * piece // per_row

    def fill(low_ref, high_ref):
        @pl.loop(0, mine_ref.shape[0] // block)
        def _(step):
            for i in range(block):
                for q, source in enumerate((low_ref, high_ref)):
                    at = (2 * i + q) * piece
                    lines[at : at + piece, :] = source[step * block + i].astype(jnp.float32)
            for group in range(0, rows, 8):
                lanes = [
                    lines[pl.ds(group * per_row + lane, 8, stride=per_row), :] for lane in range(per_row)
                ]
                at = pl.ds(pl.multiple_of(step * rows + group, 8), 8)
                out_ref[at, :] = jnp.concatenate(lanes, axis=1).astype(jnp.bfloat16)

    @pl.when(core_ref[0] == 0)
    def _():
        fill(mine_ref, twin_ref)

    @pl.when(core_ref[0] != 0)
    def _():
        fill(twin_ref, mine_ref)


def lay(core, mine, twin, shape):
    whole = pl.BlockSpec(memory_space=pltpu.VMEM)
    return pl.pallas_call(
        lay_kernel,
        out_shape=jax.ShapeDtypeStruct(shape, jnp.bfloat16),
        in_specs=[pl.BlockSpec(memory_space=pltpu.SMEM), whole, whole],
        out_specs=whole,
        scratch_shapes=[pltpu.VMEM((16 * mine.shape[1], 128), jnp.float32)],
        compiler_params=pltpu.CompilerParams(vmem_limit_bytes=4 << 20),
        name="lay",
    )(core.reshape(1).astype(jnp.int32), mine, twin)


def join_kernel(*refs):
    count = len(refs) - 2
    blocks, out_ref, arrived = refs[:count], refs[count], refs[count + 1]
    copies, at = [], 0
    for i, block in enumerate(blocks):
        size_here = block.shape[0]
        copies.append(
            pltpu.make_async_copy(block, out_ref.at[pl.ds(at, size_here), :], arrived.at[i])
        )
        copies[-1].start()
        at += size_here
    for copy in copies:
        copy.wait()


def join(blocks):
    rows, width = sum(b.shape[0] for b in blocks), blocks[0].shape[1]
    return pl.pallas_call(
        join_kernel,
        out_shape=jax.ShapeDtypeStruct((rows, width), blocks[0].dtype),
        in_specs=[pl.BlockSpec(memory_space=pl.ANY)] * len(blocks),
        out_specs=pl.BlockSpec(memory_space=pltpu.VMEM),
        scratch_shapes=[pltpu.SemaphoreType.DMA((len(blocks),))],
        compiler_params=pltpu.CompilerParams(vmem_limit_bytes=8 << 20),
        cost_estimate=pl.CostEstimate(
            flops=rows * width, bytes_accessed=4 * rows * width, transcendentals=0
        ),
        name="join",
    )(*blocks)


def step(hidden, resid, target, w_out, signs, m_old, v_old):
    features, _ = w_out.shape
    tokens = hidden.shape[0]
    group = tokens * lax.axis_size("x")
    half = lax.axis_index("yh")
    core = lax.axis_index("c")
    col = lax.axis_index("x")

    cutoff = tokens // 2
    top, low = hidden[:cutoff], hidden[cutoff:]
    left_top = shift(top, "x", 1)
    right_low = shift(low, "x", -1)
    left_low = shift(low, "x", 1)
    right_top = shift(top, "x", -1)
    far_top = shift(left_top, "x", 1)
    far_low = shift(right_low, "x", -1)

    part = shift(pack(core, w_out, signs), "yh", 1)

    other_gaps = gap((1 - half) * group, col, resid, target, group, jnp.bfloat16)
    other_gaps = shift(other_gaps, "yh", 1)
    twin = shift(part, "c", 1)
    probes = unpack_signs(signs)
    own_stack = jnp.concatenate([w_out, probes], axis=0)
    own_gaps = gap(half * group, col, resid, target, group, jnp.float32)
    other_stack = unpack(core, part, twin, signs.shape[0])

    def run(stacked, gaps, block):
        here = gaps[:, : block.shape[0]] if block.shape[0] > tokens else gaps[:, -tokens:]
        forward = lax.dot_general(
            stacked, block, (((1,), (1,)), ((), ())), preferred_element_type=jnp.float32
        )
        misfit = here.astype(jnp.float32) + forward[:features]
        spread = 1.0 + misfit * misfit
        rooted = jnp.sqrt(spread)
        slopes = (misfit / rooted).astype(jnp.bfloat16)
        bends = (forward[features:] / (spread * rooted)).astype(jnp.bfloat16)
        away = jnp.where(core == 0, bends, slopes)
        kept = jnp.where(core == 0, slopes, bends)
        away, kept = lax.optimization_barrier((away, kept))
        return [jnp.dot(terms, block, preferred_element_type=jnp.float32) for terms in (away, kept)]

    near = join((left_top, left_low, hidden, right_top, right_low))
    own_away, own_kept = run(own_stack, own_gaps, near)
    other_away, other_kept = run(other_stack, other_gaps, near)
    own_away, own_kept, other_away, other_kept, far_top, far_low = lax.optimization_barrier(
        (own_away, own_kept, other_away, other_kept, far_top, far_low)
    )
    far = join((far_top, far_low))
    own_far = run(own_stack, own_gaps, far)
    own_got = shift(own_away + own_far[0], "c", 1)
    other_far = run(other_stack, other_gaps, far)
    other_got = shift(other_away + other_far[0], "c", 1)
    pieces = cut(half, (own_kept, own_far[1], own_got, other_kept, other_far[1], other_got), 64)

    each = m_old.shape[0]
    row_start = (
        (lax.axis_index("yl") * lax.axis_size("z") + lax.axis_index("z")) * 2 + core
    ) * each
    my_probes = lax.dynamic_slice_in_dim(unpack_signs(signs).reshape(-1, 128), row_start, each, 0)
    own_rows = lax.dynamic_slice_in_dim(w_out.reshape(-1, 128), row_start, each, 0)
    terms = lax.all_to_all(pieces, ("yh", "yl", "z"), 0, 0, tiled=True)
    terms, my_probes, own_rows = lax.optimization_barrier((terms, my_probes, own_rows))
    total = jnp.sum(terms.astype(jnp.float32), axis=0)
    keep_rows = lax.dynamic_slice_in_dim(total, core * each, each, 0)
    send_rows = lax.dynamic_slice_in_dim(total, (1 - core) * each, each, 0)
    got_rows = shift(send_rows, "c", 1)
    grad_mine = jnp.where(core == 0, keep_rows, got_rows)
    curve_mine = jnp.where(core == 0, got_rows, keep_rows)

    scaling = 1.0 / math.sqrt(tokens * 512)
    gradient = grad_mine * scaling
    curvature = curve_mine * scaling
    diag_est = my_probes.astype(jnp.float32) * curvature
    new_m = beta_one * m_old + (1.0 - beta_one) * gradient
    new_v = beta_two * v_old + (1.0 - beta_two) * diag_est * diag_est
    first_fix = 1.0 - beta_one**OPT_STEP
    second_fix = 1.0 - beta_two**OPT_STEP
    update = new_m / first_fix / (jnp.sqrt(new_v / second_fix) + epsilon)
    fresh = (own_rows.astype(jnp.float32) - learn_rate * update).astype(jnp.bfloat16)

    spread_rows = jnp.broadcast_to(fresh[None], (32, *fresh.shape))
    mine_rows = lax.all_to_all(spread_rows, ("yl", "z"), 0, 0, tiled=True)
    twin_rows = shift(mine_rows, "c", 1)
    new_w = lay(core, mine_rows, twin_rows, w_out.shape)
    return (new_w, new_m, new_v)


def solution(mesh):
    fine = Mesh(mesh.devices.reshape(4, 8, 2, 2, 4), ("yl", "z", "c", "yh", "x"))
    dp, shard = ("yl", "z", "c"), ("yh", "x")
    return jax.shard_map(
        step,
        mesh=fine,
        in_specs=(
            P(dp + shard, None),
            P(shard, dp),
            P(shard, dp),
            P(shard, None),
            P(shard, None),
            P(shard + dp, None),
            P(shard + dp, None),
        ),
        out_specs=(P(shard, None), P(shard + dp, None), P(shard + dp, None)),
        check_vma=False,
    )
```

```python
import functools
import math

import jax
import jax.numpy as jnp
from jax import lax
from jax.experimental import pallas as pl
from jax.experimental.pallas import tpu as pltpu
from jax.sharding import Mesh, PartitionSpec as P


OPT_STEP = 10


beta_one = 0.9
beta_two = 0.999
learn_rate = 0.15
epsilon = 0.0001


def size(axis):
    return 8 if axis == "y" else lax.axis_size(axis)


def shift(value, axis, by):
    n = size(axis)
    hops = [(i, (i + by) % n) for i in range(n)]
    if axis == "y":
        at = [2 * (y % 4) + y // 4 for y in range(n)]
        return lax.ppermute(value, ("yl", "yh"), [(at[i], at[j]) for i, j in hops])
    return lax.ppermute(value, axis, hops)


def unpack_signs(signs):
    shifts = jnp.arange(32, dtype=jnp.int32)
    bit_values = jnp.bitwise_and(jnp.right_shift(signs[:, None, :], shifts[None, :, None]), 1)
    return (1 - 2 * bit_values).reshape(signs.shape[0] * 32, signs.shape[1]).astype(jnp.bfloat16)


def cut_kernel(half_ref, *refs):
    out_ref, lines = refs[6:]
    piece = out_ref.shape[1]
    per_row = refs[0].shape[1] // 128
    block = 8 * piece // per_row
    steps = refs[0].shape[0] // block

    for part in range(2):
        near_ref, far_ref, got_ref = refs[3 * part : 3 * part + 3]
        side = half_ref[0] if part == 0 else 1 - half_ref[0]

        @pl.loop(0, steps)
        def _(step):
            base = pl.multiple_of(step * block, 8)
            for group in range(0, block, 8):
                at = pl.ds(base + group, 8)
                rows = near_ref[at, :] + far_ref[at, :] + got_ref[at, :]
                for lane in range(per_row):
                    lines[pl.ds(group * per_row + lane, 8, stride=per_row), :] = rows[
                        :, lane * 128 : (lane + 1) * 128
                    ]
            for i in range(8):
                out_ref[(side * steps + step) * 8 + i] = lines[i * piece : (i + 1) * piece, :].astype(
                    jnp.bfloat16
                )


def cut(half, terms, plane):
    cells = 2 * terms[0].size
    piece = cells // (plane * 128)
    whole = pl.BlockSpec(memory_space=pltpu.VMEM)
    return pl.pallas_call(
        cut_kernel,
        out_shape=jax.ShapeDtypeStruct((plane, piece, 128), jnp.bfloat16),
        in_specs=[pl.BlockSpec(memory_space=pltpu.SMEM)] + [whole] * 6,
        out_specs=whole,
        scratch_shapes=[pltpu.VMEM((8 * piece, 128), jnp.float32)],
        compiler_params=pltpu.CompilerParams(vmem_limit_bytes=20 << 20),
        cost_estimate=pl.CostEstimate(flops=2 * cells, bytes_accessed=14 * cells, transcendentals=0),
        name="cut",
    )(half.reshape(1).astype(jnp.int32), *terms)


def pack_kernel(core_ref, weights_ref, signs_ref, out_ref):
    core, words = core_ref[0], signs_ref.shape[0]
    rows = out_ref.shape[0] - 2 * words
    out_ref[:rows, :] = weights_ref[pl.ds(pl.multiple_of(core * rows, 16), rows), :]
    for p in range(2):
        octet = jnp.right_shift(signs_ref[...], 16 * core + 8 * p) & 255
        out_ref[rows + p * words : rows + (p + 1) * words, :] = octet.astype(jnp.float32).astype(
            jnp.bfloat16
        )


def pack(core, weights, signs):
    rows = weights.shape[0] // 2 + 2 * signs.shape[0]
    whole = pl.BlockSpec(memory_space=pltpu.VMEM)
    return pl.pallas_call(
        pack_kernel,
        out_shape=jax.ShapeDtypeStruct((rows, weights.shape[1]), jnp.bfloat16),
        in_specs=[pl.BlockSpec(memory_space=pltpu.SMEM), whole, whole],
        out_specs=whole,
        compiler_params=pltpu.CompilerParams(vmem_limit_bytes=4 << 20),
        cost_estimate=pl.CostEstimate(
            flops=weights.size, bytes_accessed=2 * weights.size, transcendentals=0
        ),
        name="pack",
    )(core.reshape(1).astype(jnp.int32), weights, signs)


def unpack_kernel(words, core_ref, part_ref, twin_ref, out_ref):
    first = core_ref[0] == 0
    rows = part_ref.shape[0] - 2 * words
    width = part_ref.shape[1]

    def fill(low_ref, high_ref):
        out_ref[:rows, :] = low_ref[:rows, :]
        out_ref[rows : 2 * rows, :] = high_ref[:rows, :]
        place_in_byte = lax.broadcasted_iota(jnp.int32, (8, width), 0)
        for k in range(words):
            for q, source in enumerate((low_ref, high_ref)):
                signs = []
                for p in range(2):
                    at = rows + p * words + k
                    octet = source[at : at + 1, :].astype(jnp.float32).astype(jnp.int32)
                    bits = jnp.right_shift(jnp.broadcast_to(octet, (8, width)), place_in_byte) & 1
                    signs.append((1 - 2 * bits).astype(jnp.float32))
                base = 2 * rows + 32 * k + 16 * q
                out_ref[base : base + 16, :] = jnp.concatenate(signs, axis=0).astype(jnp.bfloat16)

    @pl.when(first)
    def _():
        fill(part_ref, twin_ref)

    @pl.when(jnp.logical_not(first))
    def _():
        fill(twin_ref, part_ref)


def unpack(core, part, twin, words):
    rows = 2 * (part.shape[0] - 2 * words) + 32 * words
    whole = pl.BlockSpec(memory_space=pltpu.VMEM)
    return pl.pallas_call(
        functools.partial(unpack_kernel, words),
        out_shape=jax.ShapeDtypeStruct((rows, part.shape[1]), jnp.bfloat16),
        in_specs=[pl.BlockSpec(memory_space=pltpu.SMEM), whole, whole],
        out_specs=whole,
        compiler_params=pltpu.CompilerParams(vmem_limit_bytes=6 << 20),
        cost_estimate=pl.CostEstimate(
            flops=8 * part.size, bytes_accessed=6 * part.size, transcendentals=0
        ),
        name="unpack",
    )(core.reshape(1).astype(jnp.int32), part, twin)


def gap_kernel(spot_ref, resid_ref, target_ref, own_ref, other_ref):
    half, col = spot_ref[0], spot_ref[1]
    tokens = own_ref.shape[1] // 4
    for at, out_ref in ((half, own_ref), (1 - half, other_ref)):
        for j in range(4):
            start = at * 4 * tokens + lax.rem(col + 3 + j, 4) * tokens
            cols = pl.ds(pl.multiple_of(start, 128), tokens)
            gaps = resid_ref[:, cols].astype(jnp.float32) - target_ref[:, cols].astype(jnp.float32)
            out_ref[:, j * tokens : (j + 1) * tokens] = gaps.astype(out_ref.dtype)


def gap_pair(half, col, resid, target, group):
    whole = pl.BlockSpec(memory_space=pltpu.VMEM)
    shape = (resid.shape[0], group)
    return pl.pallas_call(
        gap_kernel,
        out_shape=[jax.ShapeDtypeStruct(shape, kind) for kind in (jnp.float32, jnp.bfloat16)],
        in_specs=[pl.BlockSpec(memory_space=pltpu.SMEM), whole, whole],
        out_specs=[whole, whole],
        compiler_params=pltpu.CompilerParams(vmem_limit_bytes=6 << 20),
        cost_estimate=pl.CostEstimate(
            flops=resid.size, bytes_accessed=8 * resid.size, transcendentals=0
        ),
        name="gap",
    )(jnp.stack([half, col]).astype(jnp.int32), resid, target)


def lay_kernel(core_ref, mine_ref, twin_ref, out_ref, lines):
    piece = mine_ref.shape[1]
    per_row = out_ref.shape[1] // 128
    block = 8
    rows = block * 2 * piece // per_row

    def fill(low_ref, high_ref):
        @pl.loop(0, mine_ref.shape[0] // block)
        def _(step):
            for i in range(block):
                for q, source in enumerate((low_ref, high_ref)):
                    at = (2 * i + q) * piece
                    lines[at : at + piece, :] = source[step * block + i].astype(jnp.float32)
            for group in range(0, rows, 8):
                lanes = [
                    lines[pl.ds(group * per_row + lane, 8, stride=per_row), :] for lane in range(per_row)
                ]
                at = pl.ds(pl.multiple_of(step * rows + group, 8), 8)
                out_ref[at, :] = jnp.concatenate(lanes, axis=1).astype(jnp.bfloat16)

    @pl.when(core_ref[0] == 0)
    def _():
        fill(mine_ref, twin_ref)

    @pl.when(core_ref[0] != 0)
    def _():
        fill(twin_ref, mine_ref)


def lay(core, mine, twin, shape):
    whole = pl.BlockSpec(memory_space=pltpu.VMEM)
    return pl.pallas_call(
        lay_kernel,
        out_shape=jax.ShapeDtypeStruct(shape, jnp.bfloat16),
        in_specs=[pl.BlockSpec(memory_space=pltpu.SMEM), whole, whole],
        out_specs=whole,
        scratch_shapes=[pltpu.VMEM((16 * mine.shape[1], 128), jnp.float32)],
        compiler_params=pltpu.CompilerParams(vmem_limit_bytes=4 << 20),
        name="lay",
    )(core.reshape(1).astype(jnp.int32), mine, twin)


def join_kernel(*refs):
    count = len(refs) - 2
    blocks, out_ref, arrived = refs[:count], refs[count], refs[count + 1]
    copies, at = [], 0
    for i, block in enumerate(blocks):
        size_here = block.shape[0]
        copies.append(
            pltpu.make_async_copy(block, out_ref.at[pl.ds(at, size_here), :], arrived.at[i])
        )
        copies[-1].start()
        at += size_here
    for copy in copies:
        copy.wait()


def join(blocks):
    rows, width = sum(b.shape[0] for b in blocks), blocks[0].shape[1]
    return pl.pallas_call(
        join_kernel,
        out_shape=jax.ShapeDtypeStruct((rows, width), blocks[0].dtype),
        in_specs=[pl.BlockSpec(memory_space=pl.ANY)] * len(blocks),
        out_specs=pl.BlockSpec(memory_space=pltpu.VMEM),
        scratch_shapes=[pltpu.SemaphoreType.DMA((len(blocks),))],
        compiler_params=pltpu.CompilerParams(vmem_limit_bytes=8 << 20),
        cost_estimate=pl.CostEstimate(
            flops=rows * width, bytes_accessed=4 * rows * width, transcendentals=0
        ),
        name="join",
    )(*blocks)


def step(hidden, resid, target, w_out, signs, m_old, v_old):
    features, _ = w_out.shape
    tokens = hidden.shape[0]
    group = tokens * lax.axis_size("x")
    half = lax.axis_index("yh")
    core = lax.axis_index("c")
    col = lax.axis_index("x")

    cutoff = tokens // 2
    top = hidden[:cutoff]
    later, _ = lax.optimization_barrier((hidden, top))
    low = later[cutoff:]
    left_top = shift(top, "x", 1)
    right_low = shift(low, "x", -1)
    left_low = shift(low, "x", 1)
    right_top = shift(top, "x", -1)
    far_top = shift(left_top, "x", 1)
    far_low = shift(right_low, "x", -1)

    part = shift(pack(core, w_out, signs), "yh", 1)

    own_gaps, other_gaps = gap_pair(half, col, resid, target, group)
    other_gaps = shift(other_gaps, "yh", 1)
    twin = shift(part, "c", 1)
    probes = unpack_signs(signs)
    own_stack = jnp.concatenate([w_out, probes], axis=0)
    other_stack = unpack(core, part, twin, signs.shape[0])

    def run(stacked, gaps, block):
        here = gaps[:, : block.shape[0]] if block.shape[0] > tokens else gaps[:, -tokens:]
        forward = lax.dot_general(
            stacked, block, (((1,), (1,)), ((), ())), preferred_element_type=jnp.float32
        )
        misfit = here.astype(jnp.float32) + forward[:features]
        spread = 1.0 + misfit * misfit
        rooted = jnp.sqrt(spread)
        slopes = (misfit / rooted).astype(jnp.bfloat16)
        bends = (forward[features:] / (spread * rooted)).astype(jnp.bfloat16)
        away = jnp.where(core == 0, bends, slopes)
        kept = jnp.where(core == 0, slopes, bends)
        away, kept = lax.optimization_barrier((away, kept))
        return [jnp.dot(terms, block, preferred_element_type=jnp.float32) for terms in (away, kept)]

    near = join((left_top, left_low, hidden, right_top, right_low))
    own_away, own_kept = run(own_stack, own_gaps, near)
    other_away, other_kept = run(other_stack, other_gaps, near)
    own_away, own_kept, other_away, other_kept, far_top, far_low = lax.optimization_barrier(
        (own_away, own_kept, other_away, other_kept, far_top, far_low)
    )
    far = join((far_top, far_low))
    own_far = run(own_stack, own_gaps, far)
    own_got = shift(own_away + own_far[0], "c", 1)
    other_far = run(other_stack, other_gaps, far)
    other_got = shift(other_away + other_far[0], "c", 1)
    pieces = cut(half, (own_kept, own_far[1], own_got, other_kept, other_far[1], other_got), 64)

    each = m_old.shape[0]
    row_start = (
        (lax.axis_index("yl") * lax.axis_size("z") + lax.axis_index("z")) * 2 + core
    ) * each
    my_probes = lax.dynamic_slice_in_dim(unpack_signs(signs).reshape(-1, 128), row_start, each, 0)
    own_rows = lax.dynamic_slice_in_dim(w_out.reshape(-1, 128), row_start, each, 0)
    terms = lax.all_to_all(pieces, ("yh", "yl", "z"), 0, 0, tiled=True)
    terms, my_probes, own_rows = lax.optimization_barrier((terms, my_probes, own_rows))
    total = jnp.sum(terms.astype(jnp.float32), axis=0)
    keep_rows = lax.dynamic_slice_in_dim(total, core * each, each, 0)
    send_rows = lax.dynamic_slice_in_dim(total, (1 - core) * each, each, 0)
    got_rows = shift(send_rows, "c", 1)
    grad_mine = jnp.where(core == 0, keep_rows, got_rows)
    curve_mine = jnp.where(core == 0, got_rows, keep_rows)

    scaling = 1.0 / math.sqrt(tokens * 512)
    gradient = grad_mine * scaling
    curvature = curve_mine * scaling
    diag_est = my_probes.astype(jnp.float32) * curvature
    new_m = beta_one * m_old + (1.0 - beta_one) * gradient
    new_v = beta_two * v_old + (1.0 - beta_two) * diag_est * diag_est
    first_fix = 1.0 - beta_one**OPT_STEP
    second_fix = 1.0 - beta_two**OPT_STEP
    update = new_m / first_fix / (jnp.sqrt(new_v / second_fix) + epsilon)
    fresh = (own_rows.astype(jnp.float32) - learn_rate * update).astype(jnp.bfloat16)

    spread_rows = jnp.broadcast_to(fresh[None], (32, *fresh.shape))
    mine_rows = lax.all_to_all(spread_rows, ("yl", "z"), 0, 0, tiled=True)
    twin_rows = shift(mine_rows, "c", 1)
    new_w = lay(core, mine_rows, twin_rows, w_out.shape)
    return (new_w, new_m, new_v)


def solution(mesh):
    fine = Mesh(mesh.devices.reshape(4, 8, 2, 2, 4), ("yl", "z", "c", "yh", "x"))
    dp, shard = ("yl", "z", "c"), ("yh", "x")
    return jax.shard_map(
        step,
        mesh=fine,
        in_specs=(
            P(dp + shard, None),
            P(shard, dp),
            P(shard, dp),
            P(shard, None),
            P(shard, None),
            P(shard + dp, None),
            P(shard + dp, None),
        ),
        out_specs=(P(shard, None), P(shard + dp, None), P(shard + dp, None)),
        check_vma=False,
    )
```
